256 devices in a mesh: tm: 16 (over x, z_lo), py: 4 (over y), pz: 4 (over z_hi, core).
Axes of the slice: x: 4, y: 4, z: 8 (z_hi: 2, z_lo: 4; z = z_hi * 4 + z_lo), core: 2. Of those that a mesh axis runs over, the one named last changes fastest.
Arguments:
- start_states: float32 [16, 3, 128, 8, 16, 128], P('tm', None, None, None, ('py', 'pz')), may hold values from -6 to 6
Outputs:
- new_states: float32 [16, 3, 128, 8, 16, 128], P('tm', None, None, None, ('py', 'pz'))
The draws below stay inside these ranges and needn't reach their ends.
All inputs are finite; a program needn't handle non-finite values.
Results may differ from the reference program's by a relative error of at most 0.0001.
Values sent between devices are 32-bit elements; how exact they have to be, the bound alone decides.
A program may use at most 128 MiB of HBM per device.

```python
import jax
import jax.numpy as jnp
from jax import lax

N = 128
M = 64
PEN = 16
SLICES = 16


def shard_levels(rng, shape, shards, least, high):
    level = 1.0
    for dim, shards_of in shards:
        draws = jax.random.uniform(jax.random.fold_in(jax.random.fold_in(rng, 6), dim), (shards_of,), jnp.float32, least / len(shards), high / len(shards))
        level = level * jnp.repeat(jnp.exp(draws), shape[dim] // shards_of).reshape((-1,) + (1,) * (len(shape) - 1 - dim))
    return level


def bell_draw(rng, shape, width, most, cuts=(), kind=jnp.bfloat16):
    entries = width * jax.random.normal(rng, shape, jnp.float32)
    if cuts:
        entries = entries * shard_levels(rng, shape, cuts, -0.22, 0.18)
    return jnp.clip(entries, -most, most).astype(kind)


def setup_inputs(seed: int = 0) -> dict:
    arg_keys = jax.random.split(jax.random.key(seed), 2)
    return {
        "start_states": bell_draw(arg_keys[0], (SLICES, 3, N, N // PEN, PEN, N), 1.0, 6.0, ((0, 16), (4, 16)), jnp.float32),
    }


viscosity = 0.03
time_step = 0.004


def signed_wave(length):
    places = jnp.arange(length, dtype=jnp.int32)
    return jnp.where(places < length // 2, places, places - length).astype(jnp.float32)


def wavenumbers(retained):
    wave_x = signed_wave(retained)[:, None, None]
    wave_y = signed_wave(retained)[None, :, None]
    wave_z = jnp.arange(retained // 2, dtype=jnp.int32).astype(jnp.float32)[None, None, :]
    return wave_x, wave_y, wave_z


def vorticity(coeffs, wavegrid):
    wave_x, wave_y, wave_z = wavegrid
    along_x = 1j * (wave_y * coeffs[2] - wave_z * coeffs[1])
    along_y = 1j * (wave_z * coeffs[0] - wave_x * coeffs[2])
    along_z = 1j * (wave_x * coeffs[1] - wave_y * coeffs[0])
    return jnp.stack([along_x, along_y, along_z])


def project(coeffs, wavegrid):
    wave_x, wave_y, wave_z = wavegrid
    squared = wave_x * wave_x + wave_y * wave_y + wave_z * wave_z
    divergence = (wave_x * coeffs[0] + wave_y * coeffs[1] + wave_z * coeffs[2]) / jnp.maximum(squared, 1.0)
    return jnp.stack([coeffs[0] - wave_x * divergence, coeffs[1] - wave_y * divergence, coeffs[2] - wave_z * divergence])


def cross_product(first_field, second_field):
    return jnp.stack([
        first_field[1] * second_field[2] - first_field[2] * second_field[1],
        first_field[2] * second_field[0] - first_field[0] * second_field[2],
        first_field[0] * second_field[1] - first_field[1] * second_field[0],
    ])


def widen(coeffs, extent, contracted):
    length = coeffs.shape[contracted]
    halfway = length // 2
    low_part = lax.slice_in_dim(coeffs, 0, halfway, axis=contracted)
    high_part = lax.slice_in_dim(coeffs, halfway, length, axis=contracted)
    filler_shape = list(coeffs.shape)
    filler_shape[contracted] = extent - length
    return jnp.concatenate([low_part, jnp.zeros(filler_shape, coeffs.dtype), high_part], axis=contracted)


def narrow(coeffs, kept, contracted):
    length = coeffs.shape[contracted]
    halfway = kept // 2
    low_part = lax.slice_in_dim(coeffs, 0, halfway, axis=contracted)
    high_part = lax.slice_in_dim(coeffs, length - halfway, length, axis=contracted)
    return jnp.concatenate([low_part, high_part], axis=contracted)


def widen_last(coeffs, columns):
    filler_shape = list(coeffs.shape)
    filler_shape[3] = columns - coeffs.shape[3]
    return jnp.concatenate([coeffs, jnp.zeros(filler_shape, coeffs.dtype)], axis=3)


def to_physical(coeffs, extent):
    retained = coeffs.shape[1]
    spread = widen(widen(coeffs, extent, 1), extent, 2)
    spread = widen_last(spread, extent // 2 + 1)
    spread = jnp.fft.ifft(spread, axis=1)
    spread = jnp.fft.ifft(spread, axis=2)
    constant_column = jnp.real(spread[..., :1]).astype(spread.dtype)
    spread = jnp.concatenate([constant_column, spread[..., 1:]], axis=3)
    return jnp.fft.irfft(spread, n=extent, axis=3) * (extent ** 3 / retained ** 1.5)


def to_spectral(fields, retained):
    extent = fields.shape[-1]
    spectrum = jnp.fft.rfftn(fields, axes=(1, 2, 3))
    spectrum = narrow(narrow(spectrum, retained, 1), retained, 2)[..., : retained // 2]
    return spectrum * (retained ** 1.5 / extent ** 3)


def restrict(coeffs, kept):
    return narrow(narrow(coeffs, kept, 1), kept, 2)[..., : kept // 2]


def prolong(coeffs, retained):
    wider = widen(widen(coeffs, retained, 1), retained, 2)
    return widen_last(wider, retained // 2)


def advance(coeffs):
    retained = coeffs.shape[1]
    extent = 3 * retained // 2
    wavegrid = wavenumbers(retained)
    fields = to_physical(jnp.concatenate([coeffs, vorticity(coeffs, wavegrid)], axis=0), extent)
    product = cross_product(fields[:3], fields[3:])
    nonlinear = to_spectral(product, retained)
    wave_x, wave_y, wave_z = wavegrid
    squared = wave_x * wave_x + wave_y * wave_y + wave_z * wave_z
    damping = jnp.exp(-viscosity * time_step * squared)
    return damping * (coeffs + time_step * project(nonlinear, wavegrid))


def pack(coeffs):
    merged = jnp.concatenate([jnp.real(coeffs), jnp.imag(coeffs)], axis=-1).astype(jnp.float32)
    return merged.reshape(3, N, N // PEN, PEN, N)


def unpack(stored):
    merged = stored.reshape(3, N, N, N)
    return merged[..., : N // 2] + 1j * merged[..., N // 2:]


def reference(start_states):
    slices = start_states.shape[0]
    fine_ends = []
    corrections = []
    first_state = None
    for slice_number in range(slices):
        spectral_state = project(unpack(start_states[slice_number]), wavenumbers(N))
        if slice_number == 0:
            first_state = spectral_state
        fine_end = advance(spectral_state)
        coarse_next = advance(restrict(spectral_state, M))
        fine_ends.append(fine_end)
        corrections.append(restrict(fine_end, M) - coarse_next)
    chained = restrict(fine_ends[0], M)
    packed = [pack(first_state)]
    for slice_number in range(1, slices):
        previous = fine_ends[slice_number - 1]
        upper_band = previous - prolong(restrict(previous, M), N)
        packed.append(pack(prolong(chained, N) + upper_band))
        if slice_number < slices - 1:
            chained = advance(chained) + corrections[slice_number]
    return jnp.stack(packed)
```

```python
from functools import partial
import math

import jax
import jax.numpy as jnp
from jax import lax
from jax.experimental import pallas as pl
from jax.experimental.pallas import tpu as pltpu
import numpy as np
from jax.sharding import PartitionSpec as P

M = 64


viscosity = 0.03
time_step = 0.004
highest = lax.Precision.HIGH


def items_in_groups(x, axis, split_dim, concat_dim, work, item_dim, out_dim):

    def moved(group):
        return lax.all_to_all(group, axis, split_axis=split_dim, concat_axis=concat_dim, tiled=True)

    items = jax.tree.leaves(x)[0].shape[item_dim]
    ends = [items * k // 2 for k in range(2 + 1)] if items % 2 == 0 else [0, items]
    groups = [
        jax.tree.map(lambda a: lax.slice_in_dim(a, low, high, axis=item_dim), x)
        for low, high in zip(ends, ends[1:])
    ]
    arrived = [moved(group) for group in groups]
    made = [work(group) for group in arrived]
    return jax.tree.map(lambda *parts: jnp.concatenate(parts, axis=out_dim), *made)


def shifted(block, axis, distance):
    devices = range(lax.axis_size(axis))
    route = [(i - distance, i) for i in devices if i - distance in devices]
    return lax.ppermute(block, axis, route)


def signed_wave(places, length):
    return jnp.where(places < length // 2, places, places - length)


def rotate(values):
    halfway = values.shape[-1] // 2
    return jnp.concatenate([-values[..., halfway:], values[..., :halfway]], axis=-1)


def trig_pair(outer, inner, extent, factor):
    residue = jnp.mod(outer[:, None] * inner[None, :], extent)
    radians = residue.astype(jnp.float32) * (2.0 * math.pi / extent)
    return (jnp.cos(radians) * factor, jnp.sin(radians) * factor)


def complex_apply(cosine_part, sine_part, values, contracted, direction_sign):
    kernel = jnp.stack(
        [
            jnp.stack([cosine_part, -direction_sign * sine_part]),
            jnp.stack([direction_sign * sine_part, cosine_part]),
        ]
    )
    halfway = values.shape[-1] // 2
    split = values.reshape(values.shape[:-1] + (2, halfway))
    if contracted == 1:
        pattern = "pqok,fkaqh->foaph"
    else:
        pattern = "pqok,flkqh->floph"
    result = jnp.einsum(pattern, kernel, split, precision=highest)
    return result.reshape(result.shape[:-2] + (2 * halfway,))


def inverse_z(extent, retained):
    halfway = retained // 2
    columns = jnp.arange(retained, dtype=jnp.int32)
    harmonic = columns % halfway
    weight = jnp.where(harmonic == 0, 1.0, 2.0) * retained ** (-0.5)
    residue = jnp.mod(harmonic[:, None] * jnp.arange(extent, dtype=jnp.int32)[None, :], extent)
    radians = residue.astype(jnp.float32) * (2.0 * math.pi / extent)
    return (
        jnp.where((columns < halfway)[:, None], jnp.cos(radians), -jnp.sin(radians))
        * weight[:, None]
    )


def forward_z(extent, retained):
    halfway = retained // 2
    columns = jnp.arange(retained, dtype=jnp.int32)
    harmonic = columns % halfway
    residue = jnp.mod(jnp.arange(extent, dtype=jnp.int32)[:, None] * harmonic[None, :], extent)
    radians = residue.astype(jnp.float32) * (2.0 * math.pi / extent)
    return jnp.where((columns < halfway)[None, :], jnp.cos(radians), -jnp.sin(radians)) * (
        math.sqrt(retained) / extent
    )


def inverse_tail(portion, extent, sectioned, layout):
    count_py, count_pz, groups, member = layout
    retained = portion.shape[2]
    local_rows = retained // groups
    places = jnp.arange(retained, dtype=jnp.int32)
    owners = places // local_rows
    wave_y = signed_wave(places % local_rows * groups + owners, retained)
    points = jnp.arange(extent, dtype=jnp.int32)
    cosine_part, sine_part = trig_pair(points, wave_y, extent, retained ** (-0.5))
    along_y = complex_apply(cosine_part, sine_part, portion, 2, 1.0)
    return jnp.einsum("flyr,rz->flyz", along_y, inverse_z(extent, retained), precision=highest)


def forward_tail(portion, retained, sectioned, layout):
    count_py, count_pz, groups, member = layout
    extent = portion.shape[1]
    local_rows = extent // groups
    places = jnp.arange(extent, dtype=jnp.int32)
    points = places // local_rows * local_rows + places % local_rows
    wave_x = signed_wave(jnp.arange(retained, dtype=jnp.int32), retained)
    cosine_part, sine_part = trig_pair(wave_x, points, extent, math.sqrt(retained) / extent)
    return complex_apply(cosine_part, sine_part, portion, 1, -1.0)


def to_physical(coeffs, wavegrid, extent, resolution, layout):
    wave_x, wave_y, wave_z = wavegrid
    retained = coeffs.shape[1]
    seeds = jnp.concatenate([coeffs, wave_x * coeffs[1:3]], axis=0)
    points = jnp.arange(extent, dtype=jnp.int32)
    wave_rows = signed_wave(jnp.arange(retained, dtype=jnp.int32), retained)
    cosine_part, sine_part = trig_pair(points, wave_rows, extent, retained ** (-0.5))
    moved_x = complex_apply(cosine_part, sine_part, seeds, 1, 1.0)
    curl_x = rotate(wave_y * moved_x[2] - wave_z * moved_x[1])
    curl_y = rotate(wave_z * moved_x[0] - moved_x[4])
    curl_z = rotate(moved_x[3] - wave_y * moved_x[0])
    spread = jnp.concatenate([moved_x[:3], jnp.stack([curl_x, curl_y, curl_z])], axis=0)
    if resolution == "coarse":
        finish = partial(inverse_tail, extent=extent, sectioned=False, layout=layout)
        return finish(lax.all_to_all(spread, ("py", "pz"), split_axis=1, concat_axis=2, tiled=True))
    else:
        finish = partial(inverse_tail, extent=extent, sectioned=False, layout=layout)
        return items_in_groups(spread, ("py", "pz"), 1, 2, finish, 0, 0)


def to_spectral(fields, retained, resolution, layout):
    count_py, count_pz, groups, member = layout
    extent = fields.shape[-1]
    along_z = jnp.einsum("flyz,zr->flyr", fields, forward_z(extent, retained), precision=highest)
    local_rows = retained // groups
    places = jnp.arange(retained, dtype=jnp.int32)
    wave_y = signed_wave(places % local_rows * groups + places // local_rows, retained)
    cosine_part, sine_part = trig_pair(
        wave_y, jnp.arange(extent, dtype=jnp.int32), extent, math.sqrt(retained) / extent
    )
    along_y = complex_apply(cosine_part, sine_part, along_z, 2, -1.0)
    if resolution == "coarse":
        finish = partial(forward_tail, retained=retained, sectioned=False, layout=layout)
        return finish(
            lax.all_to_all(along_y, ("py", "pz"), split_axis=2, concat_axis=1, tiled=True)
        )
    else:
        finish = partial(forward_tail, retained=retained, sectioned=False, layout=layout)
        return finish(
            lax.all_to_all(along_y, ("py", "pz"), split_axis=2, concat_axis=1, tiled=True)
        )


def wave_grid(retained, layout):
    count_py, count_pz, groups, member = layout
    places = jnp.arange(retained, dtype=jnp.int32)
    wave_x = signed_wave(places, retained).astype(jnp.float32)[:, None, None]
    local_places = jnp.arange(retained // groups, dtype=jnp.int32)
    wave_y = signed_wave(local_places * groups + member, retained).astype(jnp.float32)[
        None, :, None
    ]
    wave_z = (places % (retained // 2)).astype(jnp.float32)[None, None, :]
    return (wave_x, wave_y, wave_z)


def project(coeffs, wavegrid):
    wave_x, wave_y, wave_z = wavegrid
    squared = wave_x * wave_x + wave_y * wave_y + wave_z * wave_z
    divergence = (wave_x * coeffs[0] + wave_y * coeffs[1] + wave_z * coeffs[2]) / jnp.maximum(
        squared, 1.0
    )
    return jnp.stack(
        [
            coeffs[0] - wave_x * divergence,
            coeffs[1] - wave_y * divergence,
            coeffs[2] - wave_z * divergence,
        ]
    )


def cross_product(first_field, second_field):
    return jnp.stack(
        [
            first_field[1] * second_field[2] - first_field[2] * second_field[1],
            first_field[2] * second_field[0] - first_field[0] * second_field[2],
            first_field[0] * second_field[1] - first_field[1] * second_field[0],
        ]
    )


def advance(coeffs, resolution, layout):
    retained = coeffs.shape[1]
    extent = 3 * retained // 2
    wavegrid = wave_grid(retained, layout)
    fields = to_physical(coeffs, wavegrid, extent, resolution, layout)
    product = cross_product(fields[:3], fields[3:])
    nonlinear = to_spectral(product, retained, resolution, layout)
    wave_x, wave_y, wave_z = wavegrid
    squared = wave_x * wave_x + wave_y * wave_y + wave_z * wave_z
    damping = jnp.exp(-viscosity * time_step * squared)
    return damping * (coeffs + time_step * project(nonlinear, wavegrid))


def restrict(coeffs, kept, groups):
    halfway = kept // 2
    retained = coeffs.shape[1]
    rows_kept = jnp.concatenate([coeffs[:, :halfway], coeffs[:, retained - halfway :]], axis=1)
    local_rows = coeffs.shape[2]
    local_kept = kept // groups // 2
    rows_kept = jnp.concatenate(
        [rows_kept[:, :, :local_kept], rows_kept[:, :, local_rows - local_kept :]], axis=2
    )
    columns_half = coeffs.shape[3] // 2
    return jnp.concatenate(
        [rows_kept[..., :halfway], rows_kept[..., columns_half : columns_half + halfway]], axis=3
    )


def prolong(coeffs, retained, groups):
    components, kept, local_kept, width = coeffs.shape
    halfway = kept // 2
    zeros_x = jnp.zeros((components, retained - kept, local_kept, width), jnp.float32)
    wider = jnp.concatenate([coeffs[:, :halfway], zeros_x, coeffs[:, halfway:]], axis=1)
    local_rows = retained // groups
    split_rows = local_kept // 2
    zeros_y = jnp.zeros((components, retained, local_rows - local_kept, width), jnp.float32)
    wider = jnp.concatenate([wider[:, :, :split_rows], zeros_y, wider[:, :, split_rows:]], axis=2)
    zeros_z = jnp.zeros((components, retained, local_rows, retained // 2 - halfway), jnp.float32)
    return jnp.concatenate([wider[..., :halfway], zeros_z, wider[..., halfway:], zeros_z], axis=3)


G = 3 * M // 2
PARTS = 16
LOCAL = M // PARTS
PLANES = G // PARTS
CHUNK = LOCAL * PLANES
LANES = 128
PAIR = LANES // 2
QUAD = PAIR // 2
MESH = pl.DeviceIdType.MESH


def halves(matrix):
    high = np.asarray(matrix, np.float32).astype(jnp.bfloat16)
    low = (np.asarray(matrix, np.float32) - high.astype(np.float32)).astype(jnp.bfloat16)
    return high, low


def coarse_matrices():
    points = np.arange(G)
    waves = np.where(np.arange(M) < M // 2, np.arange(M), np.arange(M) - M)
    angle = (points[:, None] * waves[None, :]) % G * (2.0 * np.pi / G)
    spread = np.concatenate([np.cos(angle), np.sin(angle)], 1) * M**-0.5
    gather = np.concatenate([np.cos(angle.T), -np.sin(angle.T)], 1) * (M**0.5 / G)
    harmonic = np.arange(M // 2)
    angle = (points[:, None] * harmonic[None, :]) % G * (2.0 * np.pi / G)
    weight = np.where(harmonic == 0, 1.0, 2.0) * M**-0.5
    inverse = np.zeros((PAIR, LANES))
    inverse[:, :G] = np.concatenate([np.cos(angle) * weight, -np.sin(angle) * weight], 1).T
    forward = np.zeros((LANES, PAIR))
    forward[:G] = np.concatenate([np.cos(angle), -np.sin(angle)], 1) * (M**0.5 / G)
    turned = np.concatenate([-forward[:, QUAD:], forward[:, :QUAD]], 1)
    none_in = np.zeros_like(inverse)
    none_out = np.zeros_like(forward)
    inverse_pair = np.block([[inverse, none_in], [none_in, inverse]])
    forward_pair = np.block(
        [[forward, none_out, turned, none_out], [none_out, forward, none_out, turned]]
    )
    forward_one = np.concatenate([forward, forward, turned, turned], 1)
    made = []
    for matrix in (spread, gather):
        high, low = halves(matrix)
        made.append(jnp.asarray(np.concatenate([high, high, low], 1)))
    for matrix in (inverse_pair, forward_pair, forward_one):
        high, low = halves(matrix)
        made.append(jnp.asarray(np.concatenate([high, high, low], 0)))
    return made


def wave_tables(member):
    rows = signed_wave(jnp.arange(M, dtype=jnp.int32), M).astype(jnp.float32)[None, :, None]
    local = jnp.arange(LOCAL, dtype=jnp.int32)
    wave_y = signed_wave(local * PARTS + member, M).astype(jnp.float32)[:, None, None]
    lane = jnp.arange(LANES, dtype=jnp.int32)[None, None, :]
    wave_z = (lane % QUAD).astype(jnp.float32)
    full = (LOCAL, M, LANES)
    kx, ky, kz = (jnp.broadcast_to(w, full) for w in (rows, wave_y, wave_z))
    lower = lane < PAIR
    squared = kx * kx + ky * ky + kz * kz
    return (
        jnp.where(lower, kx, ky),
        ky,
        jnp.where(lower, kz, kx)[0],
        kz[0],
        1.0 / jnp.maximum(squared, 1.0),
        jnp.exp(-viscosity * time_step * squared),
    )


def turn(x):
    lane = lax.broadcasted_iota(jnp.int32, x.shape, 1)
    return jnp.where(
        lane % PAIR < QUAD, -pltpu.roll(x, LANES - QUAD, 1), pltpu.roll(x, QUAD, 1)
    )


def split(x):
    high = x.astype(jnp.bfloat16)
    return high, (x - high.astype(jnp.float32)).astype(jnp.bfloat16)


def left_apply(matrix, x):
    high, low = split(x)
    return jnp.dot(
        matrix, jnp.concatenate([high, low, high], 0), preferred_element_type=jnp.float32
    )


def right_apply(x, matrix):
    high, low = split(x)
    return jnp.dot(
        jnp.concatenate([high, low, high], 1), matrix, preferred_element_type=jnp.float32
    )


def spread_waves(state, a, tables, spread):
    kxy, ky, kzx, kz = tables[0][a], tables[1][a], tables[2][...], tables[3][...]
    first, third = state[a, :, :LANES], state[a, :, LANES:]
    lower = lax.broadcasted_iota(jnp.int32, first.shape, 1) < PAIR
    raw_one = ky * third - kz * first
    raw_two = kzx * first - kxy * jnp.where(lower, third, pltpu.roll(first, PAIR, 1))
    fields = jnp.concatenate(
        [first, jnp.where(lower, third, turn(raw_one)), turn(raw_two)], 1
    )
    turned = jnp.concatenate(
        [turn(first), jnp.where(lower, turn(third), -raw_one), -raw_two], 1
    )
    return left_apply(spread, jnp.concatenate([fields, turned], 0))


def plane_product(fetched, x, mats):
    spread, gather, inverse_pair, forward_pair, forward_one = mats
    fields, turned = [], []
    for g in range(3):
        rows = jnp.concatenate(
            [fetched[g, pl.ds(LOCAL * x + a, PARTS, stride=CHUNK), :] for a in range(LOCAL)], 0
        )
        fields.append(rows)
        turned.append(turn(rows))
    along_y = left_apply(
        spread, jnp.concatenate([jnp.concatenate(fields, 1), jnp.concatenate(turned, 1)], 0)
    )
    grids = [
        right_apply(along_y[:, LANES * g : LANES * (g + 1)], inverse_pair) for g in range(3)
    ]
    u0, u1 = grids[0][:, :LANES], grids[0][:, LANES:]
    u2, w0 = grids[1][:, :LANES], grids[1][:, LANES:]
    w1, w2 = grids[2][:, :LANES], grids[2][:, LANES:]
    pair = jnp.concatenate([u1 * w2 - u2 * w1, u2 * w0 - u0 * w2], 1)
    back_pair = right_apply(pair, forward_pair)
    back_one = right_apply(u0 * w1 - u1 * w0, forward_one)
    return left_apply(
        gather,
        jnp.concatenate(
            [
                jnp.concatenate([back_pair[:, :LANES], back_one[:, :LANES]], 1),
                jnp.concatenate([back_pair[:, LANES:], back_one[:, LANES:]], 1),
            ],
            0,
        ),
    )


def gather_waves(fetched, state, a, tables, gather):
    kxy, kz, inverse, damping = tables[0][a], tables[3][...], tables[4][a], tables[5][a]
    rows = [fetched[g, pl.ds(a, G, stride=LOCAL), :] for g in range(2)]
    turned = [turn(r) for r in rows]
    modes = left_apply(
        gather, jnp.concatenate([jnp.concatenate(rows, 1), jnp.concatenate(turned, 1)], 0)
    )
    first, third = modes[:, :LANES], modes[:, LANES:]
    along = kxy * first
    divergence = (along + pltpu.roll(along, PAIR, 1) + kz * third) * inverse
    return (
        damping * (state[a, :, :LANES] + time_step * (first - kxy * divergence)),
        damping * (state[a, :, LANES:] + time_step * (third - kz * divergence)),
    )


def chain_kernel(
    payload,
    kxy, ky, kzx, kz, inverse, damping,
    spread, gather, inverse_pair, forward_pair, forward_one,
    result,
    states, terms, out_f, in_f, out_b, in_b,
    term_send, term_recv, state_send, state_recv, f_send, f_recv, b_send, b_recv,
):
    tables = (kxy, ky, kzx, kz, inverse, damping)
    mats = tuple(m[...] for m in (spread, gather, inverse_pair, forward_pair, forward_one))
    slot, py, pz = lax.axis_index("tm"), lax.axis_index("py"), lax.axis_index("pz")
    slices = lax.axis_size("tm")
    stride = slices // 4
    far, core = pz // 2, pz % 2
    is_chain = (far == 0) & (slot % stride == 0) & (slot < 2 * stride)
    own_term = (slot == 0) & (far == 0)
    sends_term = jnp.logical_not(own_term) & (slot < slices - 1)
    side = slot // stride
    me = py * 4 + side * 2 + core

    def term_copy(source_slice):
        return pltpu.make_async_remote_copy(
            src_ref=payload,
            dst_ref=terms.at[source_slice],
            send_sem=term_send,
            recv_sem=term_recv.at[source_slice],
            device_id=(far * stride, py, core),
            device_id_type=MESH,
        )

    def state_copy(t):
        return pltpu.make_async_remote_copy(
            src_ref=states.at[t],
            dst_ref=result,
            send_sem=state_send.at[t],
            recv_sem=state_recv,
            device_id=(t, py, side * 2 + core),
            device_id_type=MESH,
        )

    def part_copy(source, target, sends, recvs, owner, peer):
        return pltpu.make_async_remote_copy(
            src_ref=source.at[:, pl.ds(pl.multiple_of(peer * CHUNK, 8), CHUNK), :],
            dst_ref=target.at[:, pl.ds(pl.multiple_of(owner * CHUNK, 8), CHUNK), :],
            send_sem=sends.at[peer],
            recv_sem=recvs.at[owner],
            device_id=((peer // 2) % 2 * stride, peer // 4, peer % 2),
            device_id_type=MESH,
        )

    def exchange(source, target, sends, recvs):
        def send(j, carried):
            peer = (me + j) % PARTS
            part_copy(source, target, sends, recvs, me, peer).start()
            return carried

        def receive(j, carried):
            peer = (me + PARTS - j) % PARTS
            part_copy(source, target, sends, recvs, peer, peer).wait_recv()
            return carried

        def finish(j, carried):
            peer = (me + j) % PARTS
            part_copy(source, target, sends, recvs, me, peer).wait_send()
            return carried

        lax.fori_loop(1, PARTS, send, 0)
        mine = pl.ds(pl.multiple_of(me * CHUNK, 8), CHUNK)
        target[:, mine, :] = source[:, mine, :]
        lax.fori_loop(1, PARTS, receive, 0)
        lax.fori_loop(1, PARTS, finish, 0)

    @pl.when(sends_term)
    def _():
        term_copy(slot).start()

    @pl.when(slot == 0)
    def _():
        result[...] = jnp.zeros_like(result)

    @pl.when(is_chain)
    def _():
        @pl.when(own_term)
        def _():
            states[1] = payload[...]

        @pl.when(jnp.logical_not(own_term))
        def _():
            term_copy(0).wait_recv()
            states[1] = terms[0]

        def step(t, carried):
            state_copy(t).start()
            state = states.at[t]
            for a in range(LOCAL):
                waves = spread_waves(state, a, tables, mats[0])
                for g in range(3):
                    out_f[g, pl.ds(a, G, stride=LOCAL), :] = waves[:, LANES * g : LANES * (g + 1)]
            exchange(out_f, in_f, f_send, f_recv)
            for x in range(PLANES):
                back = plane_product(in_f, x, mats)
                for g in range(2):
                    for a in range(LOCAL):
                        out_b[g, pl.ds(LOCAL * x + a, PARTS, stride=CHUNK), :] = back[
                            PARTS * a : PARTS * (a + 1), LANES * g : LANES * (g + 1)
                        ]
            exchange(out_b, in_b, b_send, b_recv)
            term_copy(t).wait_recv()
            for a in range(LOCAL):
                first, third = gather_waves(in_b, state, a, tables, mats[1])
                states[t + 1, a, :, :LANES] = first + terms[t, a, :, :LANES]
                states[t + 1, a, :, LANES:] = third + terms[t, a, :, LANES:]
            return carried

        lax.fori_loop(1, slices - 1, step, 0)
        state_copy(slices - 1).start()

        def finish(t, carried):
            state_copy(t).wait_send()
            return carried

        lax.fori_loop(1, slices, finish, 0)

    @pl.when(sends_term)
    def _():
        term_copy(slot).wait_send()

    @pl.when(slot != 0)
    def _():
        state_copy(slot).wait_recv()


def chain(payload, slices):
    core = lax.axis_index("pz") % 2
    side = lax.axis_index("tm") // (slices // 4) % 2
    member = lax.axis_index("py") * 4 + side * 2 + core
    packed = payload.transpose(2, 1, 0, 3)
    packed = jnp.concatenate([packed, packed[:, :, 2:]], axis=2).reshape(LOCAL, M, 2 * LANES)
    vmem = pl.BlockSpec(memory_space=pltpu.VMEM)
    operands = [packed, *wave_tables(member), *coarse_matrices()]
    block = (LOCAL, M, 2 * LANES)
    made = pl.pallas_call(
        chain_kernel,
        out_shape=jax.ShapeDtypeStruct(block, jnp.float32),
        in_specs=[vmem] * len(operands),
        out_specs=vmem,
        scratch_shapes=[
            pltpu.VMEM((slices,) + block, jnp.float32),
            pltpu.VMEM((slices,) + block, jnp.float32),
            pltpu.VMEM((3, G * LOCAL, LANES), jnp.float32),
            pltpu.VMEM((3, G * LOCAL, LANES), jnp.float32),
            pltpu.VMEM((2, G * LOCAL, LANES), jnp.float32),
            pltpu.VMEM((2, G * LOCAL, LANES), jnp.float32),
            pltpu.SemaphoreType.DMA,
            pltpu.SemaphoreType.DMA((slices,)),
            pltpu.SemaphoreType.DMA((slices,)),
            pltpu.SemaphoreType.DMA,
            pltpu.SemaphoreType.DMA((PARTS,)),
            pltpu.SemaphoreType.DMA((PARTS,)),
            pltpu.SemaphoreType.DMA((PARTS,)),
            pltpu.SemaphoreType.DMA((PARTS,)),
        ],
        compiler_params=pltpu.CompilerParams(
            has_side_effects=True, vmem_limit_bytes=32 * 1024 * 1024
        ),
    )(*operands)
    return made.reshape(LOCAL, M, 4, PAIR)[:, :, :3].transpose(2, 1, 0, 3)


def shards(start_states):
    count_py = lax.axis_size("py")
    count_pz = lax.axis_size("pz")
    groups = count_py * count_pz
    member = lax.axis_index("py") * count_pz + lax.axis_index("pz")
    layout = (count_py, count_pz, groups, member)
    position = lax.axis_index("tm")
    slices = lax.axis_size("tm")
    retained = start_states.shape[-1]
    stored = start_states.reshape(3, retained, start_states.shape[3], retained)
    spectral_state = project(stored, wave_grid(retained, layout))
    fine_end = advance(spectral_state, "fine", layout)
    coarse_start = restrict(spectral_state, M, groups)
    coarse_next = advance(coarse_start, "coarse", layout)
    fine_low = restrict(fine_end, M, groups)
    correction = fine_low - coarse_next
    payload = jnp.where(position == 0, fine_low, correction)
    current = chain(payload, slices)
    upper_band = fine_end - prolong(fine_low, retained, groups)
    previous = shifted(upper_band, "tm", 1)
    updated = prolong(current, retained, groups) + previous
    result = jnp.where(position == 0, spectral_state, updated)
    return result.reshape(1, result.shape[0], retained, result.shape[2], 1, retained)


def solution(mesh):
    in_specs = (P("tm", None, None, None, ("py", "pz"), None),)
    out_specs = P("tm", None, None, None, ("py", "pz"), None)
    return jax.shard_map(shards, mesh=mesh, in_specs=in_specs, out_specs=out_specs, check_vma=False)
```

```python
from functools import partial
import math

import jax
import jax.numpy as jnp
from jax import lax
from jax.experimental import pallas as pl
from jax.experimental.pallas import tpu as pltpu
import numpy as np
from jax.sharding import PartitionSpec as P

M = 64


viscosity = 0.03
time_step = 0.004
highest = lax.Precision.HIGH


def signed_wave(places, length):
    return jnp.where(places < length // 2, places, places - length)


def rotate(values):
    halfway = values.shape[-1] // 2
    return jnp.concatenate([-values[..., halfway:], values[..., :halfway]], axis=-1)


def trig_pair(outer, inner, extent, factor):
    residue = jnp.mod(outer[:, None] * inner[None, :], extent)
    radians = residue.astype(jnp.float32) * (2.0 * math.pi / extent)
    return (jnp.cos(radians) * factor, jnp.sin(radians) * factor)


def complex_apply(cosine_part, sine_part, values, contracted, direction_sign):
    kernel = jnp.stack(
        [
            jnp.stack([cosine_part, -direction_sign * sine_part]),
            jnp.stack([direction_sign * sine_part, cosine_part]),
        ]
    )
    halfway = values.shape[-1] // 2
    split = values.reshape(values.shape[:-1] + (2, halfway))
    if contracted == 1:
        pattern = "pqok,fkaqh->foaph"
    else:
        pattern = "pqok,flkqh->floph"
    result = jnp.einsum(pattern, kernel, split, precision=highest)
    return result.reshape(result.shape[:-2] + (2 * halfway,))


def inverse_z(extent, retained):
    halfway = retained // 2
    columns = jnp.arange(retained, dtype=jnp.int32)
    harmonic = columns % halfway
    weight = jnp.where(harmonic == 0, 1.0, 2.0) * retained ** (-0.5)
    residue = jnp.mod(harmonic[:, None] * jnp.arange(extent, dtype=jnp.int32)[None, :], extent)
    radians = residue.astype(jnp.float32) * (2.0 * math.pi / extent)
    return (
        jnp.where((columns < halfway)[:, None], jnp.cos(radians), -jnp.sin(radians))
        * weight[:, None]
    )


def forward_z(extent, retained):
    halfway = retained // 2
    columns = jnp.arange(retained, dtype=jnp.int32)
    harmonic = columns % halfway
    residue = jnp.mod(jnp.arange(extent, dtype=jnp.int32)[:, None] * harmonic[None, :], extent)
    radians = residue.astype(jnp.float32) * (2.0 * math.pi / extent)
    return jnp.where((columns < halfway)[None, :], jnp.cos(radians), -jnp.sin(radians)) * (
        math.sqrt(retained) / extent
    )


def inverse_tail(portion, extent, sectioned, layout):
    count_py, count_pz, groups, member = layout
    retained = portion.shape[2]
    local_rows = retained // groups
    places = jnp.arange(retained, dtype=jnp.int32)
    owners = places // local_rows
    wave_y = signed_wave(places % local_rows * groups + owners, retained)
    points = jnp.arange(extent, dtype=jnp.int32)
    cosine_part, sine_part = trig_pair(points, wave_y, extent, retained ** (-0.5))
    along_y = complex_apply(cosine_part, sine_part, portion, 2, 1.0)
    return jnp.einsum("flyr,rz->flyz", along_y, inverse_z(extent, retained), precision=highest)


def forward_tail(portion, retained, sectioned, layout):
    count_py, count_pz, groups, member = layout
    extent = portion.shape[1]
    local_rows = extent // groups
    places = jnp.arange(extent, dtype=jnp.int32)
    points = places // local_rows * local_rows + places % local_rows
    wave_x = signed_wave(jnp.arange(retained, dtype=jnp.int32), retained)
    cosine_part, sine_part = trig_pair(wave_x, points, extent, math.sqrt(retained) / extent)
    return complex_apply(cosine_part, sine_part, portion, 1, -1.0)


def to_physical(coeffs, wavegrid, extent, resolution, layout):
    wave_x, wave_y, wave_z = wavegrid
    retained = coeffs.shape[1]
    seeds = jnp.concatenate([coeffs, wave_x * coeffs[1:3]], axis=0)
    points = jnp.arange(extent, dtype=jnp.int32)
    wave_rows = signed_wave(jnp.arange(retained, dtype=jnp.int32), retained)
    cosine_part, sine_part = trig_pair(points, wave_rows, extent, retained ** (-0.5))
    moved_x = complex_apply(cosine_part, sine_part, seeds, 1, 1.0)

    def arrive(part):
        return lax.all_to_all(part, ("py", "pz"), split_axis=1, concat_axis=2, tiled=True)

    finish = partial(inverse_tail, extent=extent, sectioned=False, layout=layout)
    groups = layout[2]
    places = jnp.arange(retained, dtype=jnp.int32)
    local_rows = retained // groups
    owned_y = signed_wave(places % local_rows * groups + places // local_rows, retained)
    wave_y = owned_y.astype(jnp.float32)[None, :, None]
    waves = arrive(moved_x[:3])
    slopes = arrive(moved_x[3:])
    curl_x = rotate(wave_y * waves[2] - wave_z * waves[1])
    curl_y = rotate(wave_z * waves[0] - slopes[1])
    curl_z = rotate(slopes[0] - wave_y * waves[0])
    curls = jnp.stack([curl_x, curl_y, curl_z])
    return jnp.concatenate([finish(waves), finish(curls)], axis=0)


def to_spectral(fields, retained, resolution, layout):
    count_py, count_pz, groups, member = layout
    extent = fields.shape[-1]
    along_z = jnp.einsum("flyz,zr->flyr", fields, forward_z(extent, retained), precision=highest)
    local_rows = retained // groups
    places = jnp.arange(retained, dtype=jnp.int32)
    wave_y = signed_wave(places % local_rows * groups + places // local_rows, retained)
    cosine_part, sine_part = trig_pair(
        wave_y, jnp.arange(extent, dtype=jnp.int32), extent, math.sqrt(retained) / extent
    )
    along_y = complex_apply(cosine_part, sine_part, along_z, 2, -1.0)
    if resolution == "coarse":
        finish = partial(forward_tail, retained=retained, sectioned=False, layout=layout)
        return finish(
            lax.all_to_all(along_y, ("py", "pz"), split_axis=2, concat_axis=1, tiled=True)
        )
    else:
        finish = partial(forward_tail, retained=retained, sectioned=False, layout=layout)
        return finish(
            lax.all_to_all(along_y, ("py", "pz"), split_axis=2, concat_axis=1, tiled=True)
        )


def wave_grid(retained, layout):
    count_py, count_pz, groups, member = layout
    places = jnp.arange(retained, dtype=jnp.int32)
    wave_x = signed_wave(places, retained).astype(jnp.float32)[:, None, None]
    local_places = jnp.arange(retained // groups, dtype=jnp.int32)
    wave_y = signed_wave(local_places * groups + member, retained).astype(jnp.float32)[
        None, :, None
    ]
    wave_z = (places % (retained // 2)).astype(jnp.float32)[None, None, :]
    return (wave_x, wave_y, wave_z)


def project(coeffs, wavegrid):
    wave_x, wave_y, wave_z = wavegrid
    squared = wave_x * wave_x + wave_y * wave_y + wave_z * wave_z
    divergence = (wave_x * coeffs[0] + wave_y * coeffs[1] + wave_z * coeffs[2]) / jnp.maximum(
        squared, 1.0
    )
    return jnp.stack(
        [
            coeffs[0] - wave_x * divergence,
            coeffs[1] - wave_y * divergence,
            coeffs[2] - wave_z * divergence,
        ]
    )


def cross_product(first_field, second_field):
    return jnp.stack(
        [
            first_field[1] * second_field[2] - first_field[2] * second_field[1],
            first_field[2] * second_field[0] - first_field[0] * second_field[2],
            first_field[0] * second_field[1] - first_field[1] * second_field[0],
        ]
    )


def advance(coeffs, resolution, layout):
    retained = coeffs.shape[1]
    extent = 3 * retained // 2
    wavegrid = wave_grid(retained, layout)
    fields = to_physical(coeffs, wavegrid, extent, resolution, layout)
    product = cross_product(fields[:3], fields[3:])
    nonlinear = to_spectral(product, retained, resolution, layout)
    wave_x, wave_y, wave_z = wavegrid
    squared = wave_x * wave_x + wave_y * wave_y + wave_z * wave_z
    damping = jnp.exp(-viscosity * time_step * squared)
    return damping * (coeffs + time_step * project(nonlinear, wavegrid))


def restrict(coeffs, kept, groups):
    halfway = kept // 2
    retained = coeffs.shape[1]
    rows_kept = jnp.concatenate([coeffs[:, :halfway], coeffs[:, retained - halfway :]], axis=1)
    local_rows = coeffs.shape[2]
    local_kept = kept // groups // 2
    rows_kept = jnp.concatenate(
        [rows_kept[:, :, :local_kept], rows_kept[:, :, local_rows - local_kept :]], axis=2
    )
    columns_half = coeffs.shape[3] // 2
    return jnp.concatenate(
        [rows_kept[..., :halfway], rows_kept[..., columns_half : columns_half + halfway]], axis=3
    )


def prolong(coeffs, retained, groups):
    components, kept, local_kept, width = coeffs.shape
    halfway = kept // 2
    zeros_x = jnp.zeros((components, retained - kept, local_kept, width), jnp.float32)
    wider = jnp.concatenate([coeffs[:, :halfway], zeros_x, coeffs[:, halfway:]], axis=1)
    local_rows = retained // groups
    split_rows = local_kept // 2
    zeros_y = jnp.zeros((components, retained, local_rows - local_kept, width), jnp.float32)
    wider = jnp.concatenate([wider[:, :, :split_rows], zeros_y, wider[:, :, split_rows:]], axis=2)
    zeros_z = jnp.zeros((components, retained, local_rows, retained // 2 - halfway), jnp.float32)
    return jnp.concatenate([wider[..., :halfway], zeros_z, wider[..., halfway:], zeros_z], axis=3)


G = 3 * M // 2
PARTS = 16
LOCAL = M // PARTS
PLANES = G // PARTS
CHUNK = LOCAL * PLANES
PIECES = PLANES // 2
LANES = 128
PAIR = LANES // 2
QUAD = PAIR // 2
MESH = pl.DeviceIdType.MESH


def halves(matrix):
    high = np.asarray(matrix, np.float32).astype(jnp.bfloat16)
    low = (np.asarray(matrix, np.float32) - high.astype(np.float32)).astype(jnp.bfloat16)
    return high, low


def coarse_matrices():
    points = np.arange(G)
    waves = np.where(np.arange(M) < M // 2, np.arange(M), np.arange(M) - M)
    angle = (points[:, None] * waves[None, :]) % G * (2.0 * np.pi / G)
    spread = np.concatenate([np.cos(angle), np.sin(angle)], 1) * M**-0.5
    gather = np.concatenate([np.cos(angle.T), -np.sin(angle.T)], 1) * (M**0.5 / G)
    harmonic = np.arange(M // 2)
    angle = (points[:, None] * harmonic[None, :]) % G * (2.0 * np.pi / G)
    weight = np.where(harmonic == 0, 1.0, 2.0) * M**-0.5
    inverse = np.zeros((PAIR, LANES))
    inverse[:, :G] = np.concatenate([np.cos(angle) * weight, -np.sin(angle) * weight], 1).T
    forward = np.zeros((LANES, PAIR))
    forward[:G] = np.concatenate([np.cos(angle), -np.sin(angle)], 1) * (M**0.5 / G)
    turned = np.concatenate([-forward[:, QUAD:], forward[:, :QUAD]], 1)
    none_in = np.zeros_like(inverse)
    none_out = np.zeros_like(forward)
    inverse_pair = np.block([[inverse, none_in], [none_in, inverse]])
    forward_pair = np.block(
        [[forward, none_out, turned, none_out], [none_out, forward, none_out, turned]]
    )
    forward_one = np.concatenate([forward, forward, turned, turned], 1)
    made = []
    for matrix in (spread, gather):
        high, low = halves(matrix)
        made.append(jnp.asarray(np.concatenate([high, high, low], 1)))
    for matrix in (inverse_pair, forward_pair, forward_one):
        high, low = halves(matrix)
        made.append(jnp.asarray(np.concatenate([high, high, low], 0)))
    return made


def wave_tables(member):
    rows = signed_wave(jnp.arange(M, dtype=jnp.int32), M).astype(jnp.float32)[None, :, None]
    local = jnp.arange(LOCAL, dtype=jnp.int32)
    wave_y = signed_wave(local * PARTS + member, M).astype(jnp.float32)[:, None, None]
    lane = jnp.arange(LANES, dtype=jnp.int32)[None, None, :]
    wave_z = (lane % QUAD).astype(jnp.float32)
    full = (LOCAL, M, LANES)
    kx, ky, kz = (jnp.broadcast_to(w, full) for w in (rows, wave_y, wave_z))
    lower = lane < PAIR
    squared = kx * kx + ky * ky + kz * kz
    return (
        jnp.where(lower, kx, ky),
        ky,
        jnp.where(lower, kz, kx)[0],
        kz[0],
        1.0 / jnp.maximum(squared, 1.0),
        jnp.exp(-viscosity * time_step * squared),
    )


def turn(x):
    lane = lax.broadcasted_iota(jnp.int32, x.shape, 1)
    return jnp.where(
        lane % PAIR < QUAD, -pltpu.roll(x, LANES - QUAD, 1), pltpu.roll(x, QUAD, 1)
    )


def split(x):
    high = x.astype(jnp.bfloat16)
    return high, (x - high.astype(jnp.float32)).astype(jnp.bfloat16)


def left_apply(matrix, x):
    high, low = split(x)
    return jnp.dot(
        matrix, jnp.concatenate([high, low, high], 0), preferred_element_type=jnp.float32
    )


def right_apply(x, matrix):
    high, low = split(x)
    return jnp.dot(
        jnp.concatenate([high, low, high], 1), matrix, preferred_element_type=jnp.float32
    )


def spread_waves(state, a, tables, spread):
    kxy, ky, kzx, kz = tables[0][a], tables[1][a], tables[2][...], tables[3][...]
    first, third = state[a, :, :LANES], state[a, :, LANES:]
    lower = lax.broadcasted_iota(jnp.int32, first.shape, 1) < PAIR
    raw_one = ky * third - kz * first
    raw_two = kzx * first - kxy * jnp.where(lower, third, pltpu.roll(first, PAIR, 1))
    fields = jnp.concatenate(
        [first, jnp.where(lower, third, turn(raw_one)), turn(raw_two)], 1
    )
    turned = jnp.concatenate(
        [turn(first), jnp.where(lower, turn(third), -raw_one), -raw_two], 1
    )
    return left_apply(spread, jnp.concatenate([fields, turned], 0))


def plane_product(fetched, x, mats):
    spread, gather, inverse_pair, forward_pair, forward_one = mats
    fields, turned = [], []
    for g in range(3):
        rows = jnp.concatenate(
            [fetched[g, pl.ds(LOCAL * x + a, PARTS, stride=CHUNK), :] for a in range(LOCAL)], 0
        )
        fields.append(rows)
        turned.append(turn(rows))
    along_y = left_apply(
        spread, jnp.concatenate([jnp.concatenate(fields, 1), jnp.concatenate(turned, 1)], 0)
    )
    grids = [
        right_apply(along_y[:, LANES * g : LANES * (g + 1)], inverse_pair) for g in range(3)
    ]
    u0, u1 = grids[0][:, :LANES], grids[0][:, LANES:]
    u2, w0 = grids[1][:, :LANES], grids[1][:, LANES:]
    w1, w2 = grids[2][:, :LANES], grids[2][:, LANES:]
    pair = jnp.concatenate([u1 * w2 - u2 * w1, u2 * w0 - u0 * w2], 1)
    back_pair = right_apply(pair, forward_pair)
    back_one = right_apply(u0 * w1 - u1 * w0, forward_one)
    return left_apply(
        gather,
        jnp.concatenate(
            [
                jnp.concatenate([back_pair[:, :LANES], back_one[:, :LANES]], 1),
                jnp.concatenate([back_pair[:, LANES:], back_one[:, LANES:]], 1),
            ],
            0,
        ),
    )


def gather_waves(fetched, state, a, tables, gather):
    kxy, kz, inverse, damping = tables[0][a], tables[3][...], tables[4][a], tables[5][a]
    rows = [fetched[g, pl.ds(a, G, stride=LOCAL), :] for g in range(2)]
    turned = [turn(r) for r in rows]
    modes = left_apply(
        gather, jnp.concatenate([jnp.concatenate(rows, 1), jnp.concatenate(turned, 1)], 0)
    )
    first, third = modes[:, :LANES], modes[:, LANES:]
    along = kxy * first
    divergence = (along + pltpu.roll(along, PAIR, 1) + kz * third) * inverse
    return (
        damping * (state[a, :, :LANES] + time_step * (first - kxy * divergence)),
        damping * (state[a, :, LANES:] + time_step * (third - kz * divergence)),
    )


def chain_kernel(
    low, start, fine_end,
    kxy, ky, kzx, kz, inverse, damping,
    spread, gather, inverse_pair, forward_pair, forward_one,
    result, previous,
    states, terms, term,
    own_out_f, own_in_f, own_out_b, own_in_b, out_f, in_f, out_b, in_b,
    end_send, end_recv, term_send, term_recv, state_send, state_recv,
    own_f_send, own_f_recv, own_b_send, own_b_recv, f_send, f_recv, b_send, b_recv,
):
    mats = tuple(m[...] for m in (spread, gather, inverse_pair, forward_pair, forward_one))
    slot, py, pz = lax.axis_index("tm"), lax.axis_index("py"), lax.axis_index("pz")
    slices = lax.axis_size("tm")
    stride = slices // 4
    side = slot // stride
    is_chain = (pz == 0) & (slot % stride == 0)
    own_term = (slot == 0) & (pz == 0)
    sends_term = jnp.logical_not(own_term) & (slot < slices - 1)

    def tables_of(which):
        return (kxy.at[which], ky.at[which], kzx, kz, inverse.at[which], damping.at[which])

    def slice_device(peer):
        return (slot, peer // 4, peer % 4)

    def chain_device(peer):
        return (peer % 4 * stride, peer // 4, 0)

    def term_copy(source_slice):
        return pltpu.make_async_remote_copy(
            src_ref=term,
            dst_ref=terms.at[source_slice],
            send_sem=term_send,
            recv_sem=term_recv.at[source_slice],
            device_id=(pz * stride, py, 0),
            device_id_type=MESH,
        )

    def state_copy(t):
        return pltpu.make_async_remote_copy(
            src_ref=states.at[t],
            dst_ref=result,
            send_sem=state_send.at[t],
            recv_sem=state_recv,
            device_id=(t, py, side),
            device_id_type=MESH,
        )

    def advance_into(state, tables, me, device_of, buffers, sems, write):
        out_f, in_f, out_b, in_b = buffers
        f_send, f_recv, b_send, b_recv = sems

        def part_copy(source, target, sends, recvs, k, owner, peer):
            def rows(which):
                return pl.ds(pl.multiple_of(which * CHUNK + k * 8, 8), 8)

            return pltpu.make_async_remote_copy(
                src_ref=source.at[:, rows(peer), :],
                dst_ref=target.at[:, rows(owner), :],
                send_sem=sends.at[k, peer],
                recv_sem=recvs.at[k, owner],
                device_id=device_of(peer),
                device_id_type=MESH,
            )

        def send(source, target, sends, recvs, k):
            def one(j, carried):
                part_copy(source, target, sends, recvs, k, me, (me + j) % PARTS).start()
                return carried

            lax.fori_loop(1, PARTS, one, 0)
            mine = pl.ds(pl.multiple_of(me * CHUNK + k * 8, 8), 8)
            target[:, mine, :] = source[:, mine, :]

        def receive(source, target, sends, recvs, k):
            def one(j, carried):
                peer = (me + PARTS - j) % PARTS
                part_copy(source, target, sends, recvs, k, peer, peer).wait_recv()
                return carried

            lax.fori_loop(1, PARTS, one, 0)

        def finish(source, target, sends, recvs, k):
            def one(j, carried):
                part_copy(source, target, sends, recvs, k, me, (me + j) % PARTS).wait_send()
                return carried

            lax.fori_loop(1, PARTS, one, 0)

        forth = (out_f, in_f, f_send, f_recv)
        back = (out_b, in_b, b_send, b_recv)
        for a in range(LOCAL):
            waves = spread_waves(state, a, tables, mats[0])
            for g in range(3):
                out_f[g, pl.ds(a, G, stride=LOCAL), :] = waves[:, LANES * g : LANES * (g + 1)]
        for k in range(PIECES):
            send(*forth, k)
        for k in range(PIECES):
            receive(*forth, k)
            for x in (2 * k, 2 * k + 1):
                made = plane_product(in_f, x, mats)
                for g in range(2):
                    for a in range(LOCAL):
                        out_b[g, pl.ds(LOCAL * x + a, PARTS, stride=CHUNK), :] = made[
                            PARTS * a : PARTS * (a + 1), LANES * g : LANES * (g + 1)
                        ]
            send(*back, k)
        for k in range(PIECES):
            finish(*forth, k)
        for k in range(PIECES):
            receive(*back, k)
        for a in range(LOCAL):
            write(a, *gather_waves(in_b, state, a, tables, mats[1]))
        for k in range(PIECES):
            finish(*back, k)

    end_copy = pltpu.make_async_remote_copy(
        src_ref=fine_end,
        dst_ref=previous,
        send_sem=end_send,
        recv_sem=end_recv,
        device_id=((slot + 1) % slices, py, pz),
        device_id_type=MESH,
    )

    @pl.when(slot < slices - 1)
    def _():
        end_copy.start()

    def write_term(a, first, third):
        @pl.when(slot == 0)
        def _():
            term[a] = low[a]

        @pl.when(slot != 0)
        def _():
            term[a, :, :LANES] = low[a, :, :LANES] - first
            term[a, :, LANES:] = low[a, :, LANES:] - third

    advance_into(
        start,
        tables_of(0),
        py * 4 + pz,
        slice_device,
        (own_out_f, own_in_f, own_out_b, own_in_b),
        (own_f_send, own_f_recv, own_b_send, own_b_recv),
        write_term,
    )

    @pl.when(sends_term)
    def _():
        term_copy(slot).start()

    @pl.when(slot == 0)
    def _():
        result[...] = jnp.zeros_like(result)

    @pl.when(is_chain)
    def _():
        @pl.when(own_term)
        def _():
            states[1] = term[...]

        @pl.when(jnp.logical_not(own_term))
        def _():
            term_copy(0).wait_recv()
            states[1] = terms[0]

        def step(t, carried):
            state_copy(t).start()

            def write_state(a, first, third):
                if a == 0:
                    term_copy(t).wait_recv()
                states[t + 1, a, :, :LANES] = first + terms[t, a, :, :LANES]
                states[t + 1, a, :, LANES:] = third + terms[t, a, :, LANES:]

            advance_into(
                states.at[t],
                tables_of(1),
                py * 4 + side,
                chain_device,
                (out_f, in_f, out_b, in_b),
                (f_send, f_recv, b_send, b_recv),
                write_state,
            )
            return carried

        lax.fori_loop(1, slices - 1, step, 0)
        state_copy(slices - 1).start()

        def finish_state(t, carried):
            state_copy(t).wait_send()
            return carried

        lax.fori_loop(1, slices, finish_state, 0)

    @pl.when(sends_term)
    def _():
        term_copy(slot).wait_send()

    @pl.when(slot < slices - 1)
    def _():
        end_copy.wait_send()

    @pl.when(slot != 0)
    def _():
        state_copy(slot).wait_recv()
        end_copy.wait_recv()


def packed_coarse(coeffs):
    moved = coeffs.transpose(2, 1, 0, 3)
    doubled = jnp.concatenate([moved, moved[:, :, 2:]], axis=2)
    return doubled.reshape(LOCAL, M, 2 * LANES)


def chain(low, start, fine_end, member, slices):
    chain_member = lax.axis_index("py") * 4 + lax.axis_index("tm") // (slices // 4)
    own, chained = wave_tables(member), wave_tables(chain_member)
    stacked = [
        one if n in (2, 3) else jnp.stack([one, two])
        for n, (one, two) in enumerate(zip(own, chained))
    ]
    vmem = pl.BlockSpec(memory_space=pltpu.VMEM)
    operands = [packed_coarse(low), packed_coarse(start), fine_end, *stacked, *coarse_matrices()]
    block = (LOCAL, M, 2 * LANES)
    wide = pltpu.VMEM((3, G * LOCAL, LANES), jnp.float32)
    narrow = pltpu.VMEM((2, G * LOCAL, LANES), jnp.float32)
    pieces = pltpu.SemaphoreType.DMA((PIECES, PARTS))
    anywhere = pl.BlockSpec(memory_space=pl.ANY)
    made, previous = pl.pallas_call(
        chain_kernel,
        out_shape=(
            jax.ShapeDtypeStruct(block, jnp.float32),
            jax.ShapeDtypeStruct(fine_end.shape, jnp.float32),
        ),
        in_specs=[vmem, vmem, anywhere] + [vmem] * (len(operands) - 3),
        out_specs=(vmem, anywhere),
        scratch_shapes=[
            pltpu.VMEM((slices,) + block, jnp.float32),
            pltpu.VMEM((slices,) + block, jnp.float32),
            pltpu.VMEM(block, jnp.float32),
            wide, wide, narrow, narrow,
            wide, wide, narrow, narrow,
            pltpu.SemaphoreType.DMA,
            pltpu.SemaphoreType.DMA,
            pltpu.SemaphoreType.DMA,
            pltpu.SemaphoreType.DMA((slices,)),
            pltpu.SemaphoreType.DMA((slices,)),
            pltpu.SemaphoreType.DMA,
            pieces, pieces, pieces, pieces,
            pieces, pieces, pieces, pieces,
        ],
        cost_estimate=pl.CostEstimate(
            flops=10**11, bytes_accessed=10**7, transcendentals=0
        ),
        compiler_params=pltpu.CompilerParams(
            has_side_effects=True, vmem_limit_bytes=32 * 1024 * 1024
        ),
    )(*operands)
    return made.reshape(LOCAL, M, 4, PAIR)[:, :, :3].transpose(2, 1, 0, 3), previous


def shards(start_states):
    count_py = lax.axis_size("py")
    count_pz = lax.axis_size("pz")
    groups = count_py * count_pz
    member = lax.axis_index("py") * count_pz + lax.axis_index("pz")
    layout = (count_py, count_pz, groups, member)
    position = lax.axis_index("tm")
    slices = lax.axis_size("tm")
    retained = start_states.shape[-1]
    stored = start_states.reshape(3, retained, start_states.shape[3], retained)
    spectral_state = project(stored, wave_grid(retained, layout))
    fine_end = advance(spectral_state, "fine", layout)
    coarse_start = restrict(spectral_state, M, groups)
    fine_low = restrict(fine_end, M, groups)
    current, previous = chain(fine_low, coarse_start, fine_end, member, slices)
    upper_band = previous - prolong(restrict(previous, M, groups), retained, groups)
    updated = prolong(current, retained, groups) + upper_band
    result = jnp.where(position == 0, spectral_state, updated)
    return result.reshape(1, result.shape[0], retained, result.shape[2], 1, retained)


def solution(mesh):
    in_specs = (P("tm", None, None, None, ("py", "pz"), None),)
    out_specs = P("tm", None, None, None, ("py", "pz"), None)
    return jax.shard_map(shards, mesh=mesh, in_specs=in_specs, out_specs=out_specs, check_vma=False)
```

```python
import jax
import jax.numpy as jnp
from jax import lax
from jax.experimental import pallas as pl
from jax.experimental.pallas import tpu as pltpu
import numpy as np
from jax.sharding import PartitionSpec as P

M = 64


viscosity = 0.03
time_step = 0.004


def signed_wave(places, length):
    return jnp.where(places < length // 2, places, places - length)


def restrict(coeffs, kept, groups):
    halfway = kept // 2
    retained = coeffs.shape[1]
    rows_kept = jnp.concatenate([coeffs[:, :halfway], coeffs[:, retained - halfway :]], axis=1)
    local_rows = coeffs.shape[2]
    local_kept = kept // groups // 2
    rows_kept = jnp.concatenate(
        [rows_kept[:, :, :local_kept], rows_kept[:, :, local_rows - local_kept :]], axis=2
    )
    columns_half = coeffs.shape[3] // 2
    return jnp.concatenate(
        [rows_kept[..., :halfway], rows_kept[..., columns_half : columns_half + halfway]], axis=3
    )


def prolong(coeffs, retained, groups):
    components, kept, local_kept, width = coeffs.shape
    halfway = kept // 2
    zeros_x = jnp.zeros((components, retained - kept, local_kept, width), jnp.float32)
    wider = jnp.concatenate([coeffs[:, :halfway], zeros_x, coeffs[:, halfway:]], axis=1)
    local_rows = retained // groups
    split_rows = local_kept // 2
    zeros_y = jnp.zeros((components, retained, local_rows - local_kept, width), jnp.float32)
    wider = jnp.concatenate([wider[:, :, :split_rows], zeros_y, wider[:, :, split_rows:]], axis=2)
    zeros_z = jnp.zeros((components, retained, local_rows, retained // 2 - halfway), jnp.float32)
    return jnp.concatenate([wider[..., :halfway], zeros_z, wider[..., halfway:], zeros_z], axis=3)


G = 3 * M // 2
PARTS = 16
LOCAL = M // PARTS
PLANES = G // PARTS
PIECES = PLANES // 2
FINE_LOCAL = 8
FINE_F = 5 * FINE_LOCAL
FINE_B = 3 * FINE_LOCAL
F_ROWS = 24
B_ROWS = 16
LANES = 128
PAIR = LANES // 2
QUAD = PAIR // 2
MESH = pl.DeviceIdType.MESH


def halves(matrix):
    high = np.asarray(matrix, np.float32).astype(jnp.bfloat16)
    low = (np.asarray(matrix, np.float32) - high.astype(np.float32)).astype(jnp.bfloat16)
    return high, low


def stacked(matrix, axis):
    high, low = halves(matrix)
    return jnp.asarray(np.concatenate([high, high, low], axis))


def transform_pair(retained):
    extent = 3 * retained // 2
    points = np.arange(extent)
    waves = np.where(np.arange(retained) < retained // 2, np.arange(retained), np.arange(retained) - retained)
    angle = (points[:, None] * waves[None, :]) % extent * (2.0 * np.pi / extent)
    spread = np.concatenate([np.cos(angle), np.sin(angle)], 1) * retained**-0.5
    gather = np.concatenate([np.cos(angle.T), -np.sin(angle.T)], 1) * (retained**0.5 / extent)
    return spread, gather


def depth_transforms(retained, lanes):
    extent, half = 3 * retained // 2, retained // 2
    points, harmonic = np.arange(extent), np.arange(half)
    angle = (points[:, None] * harmonic[None, :]) % extent * (2.0 * np.pi / extent)
    weight = np.where(harmonic == 0, 1.0, 2.0) * retained**-0.5
    inverse = np.zeros((retained, lanes))
    inverse[:, :extent] = np.concatenate([np.cos(angle) * weight, -np.sin(angle) * weight], 1).T
    forward = np.zeros((lanes, retained))
    forward[:extent] = np.concatenate([np.cos(angle), -np.sin(angle)], 1) * (retained**0.5 / extent)
    turned = np.concatenate([-forward[:, half:], forward[:, :half]], 1)
    return inverse, forward, turned


def coarse_matrices():
    spread, gather = transform_pair(M)
    inverse, forward, turned = depth_transforms(M, LANES)
    none_in = np.zeros_like(inverse)
    none_out = np.zeros_like(forward)
    inverse_pair = np.block([[inverse, none_in], [none_in, inverse]])
    forward_pair = np.block(
        [[forward, none_out, turned, none_out], [none_out, forward, none_out, turned]]
    )
    forward_one = np.concatenate([forward, forward, turned, turned], 1)
    order = np.concatenate([np.arange(0, G, 2), np.arange(1, G, 2)])
    gather_rows = np.concatenate([gather[:, order], gather[:, G + order]], 1)
    return [stacked(m, 1) for m in (spread, gather, spread[order], gather_rows)] + [
        stacked(m, 0) for m in (inverse_pair, forward_pair, forward_one)
    ]


def wave_tables(member):
    rows = signed_wave(jnp.arange(M, dtype=jnp.int32), M).astype(jnp.float32)[None, :, None]
    local = jnp.arange(LOCAL, dtype=jnp.int32)
    wave_y = signed_wave(local * PARTS + member, M).astype(jnp.float32)[:, None, None]
    lane = jnp.arange(LANES, dtype=jnp.int32)[None, None, :]
    wave_z = (lane % QUAD).astype(jnp.float32)
    full = (LOCAL, M, LANES)
    kx, ky, kz = (jnp.broadcast_to(w, full) for w in (rows, wave_y, wave_z))
    lower = lane < PAIR
    squared = kx * kx + ky * ky + kz * kz
    return (
        jnp.where(lower, kx, ky),
        ky,
        jnp.where(lower, kz, kx)[0],
        kz[0],
        1.0 / jnp.maximum(squared, 1.0),
        jnp.exp(-viscosity * time_step * squared),
    )


def turn(x):
    lane = lax.broadcasted_iota(jnp.int32, x.shape, 1)
    return jnp.where(
        lane % PAIR < QUAD, -pltpu.roll(x, LANES - QUAD, 1), pltpu.roll(x, QUAD, 1)
    )


def split(x):
    high = x.astype(jnp.bfloat16)
    return high, (x - high.astype(jnp.float32)).astype(jnp.bfloat16)


def left_apply(matrix, x):
    high, low = split(x)
    return jnp.dot(
        matrix, jnp.concatenate([high, low, high], 0), preferred_element_type=jnp.float32
    )


def right_apply(x, matrix):
    high, low = split(x)
    return jnp.dot(
        jnp.concatenate([high, low, high], 1), matrix, preferred_element_type=jnp.float32
    )


def spread_waves(state, a, tables, spread):
    kxy, ky, kzx, kz = tables[0][a], tables[1][a], tables[2][...], tables[3][...]
    first, third = state[a, :, :LANES], state[a, :, LANES:]
    lower = lax.broadcasted_iota(jnp.int32, first.shape, 1) < PAIR
    raw_one = ky * third - kz * first
    raw_two = kzx * first - kxy * jnp.where(lower, third, pltpu.roll(first, PAIR, 1))
    fields = jnp.concatenate(
        [first, jnp.where(lower, third, turn(raw_one)), turn(raw_two)], 1
    )
    turned = jnp.concatenate(
        [turn(first), jnp.where(lower, turn(third), -raw_one), -raw_two], 1
    )
    return left_apply(spread, jnp.concatenate([fields, turned], 0))


def plane_product(fetched, x, mats):
    spread, gather, inverse_pair, forward_pair, forward_one = mats
    fields, turned = [], []
    for g in range(3):
        rows = jnp.concatenate(
            [
                fetched[
                    pl.ds(
                        F_ROWS * (x // 2) + 8 * g + LOCAL * (x % 2) + a,
                        PARTS,
                        stride=F_ROWS * PIECES,
                    ),
                    :,
                ]
                for a in range(LOCAL)
            ],
            0,
        )
        fields.append(rows)
        turned.append(turn(rows))
    along_y = left_apply(
        spread, jnp.concatenate([jnp.concatenate(fields, 1), jnp.concatenate(turned, 1)], 0)
    )
    grids = [
        right_apply(along_y[:, LANES * g : LANES * (g + 1)], inverse_pair) for g in range(3)
    ]
    u0, u1 = grids[0][:, :LANES], grids[0][:, LANES:]
    u2, w0 = grids[1][:, :LANES], grids[1][:, LANES:]
    w1, w2 = grids[2][:, :LANES], grids[2][:, LANES:]
    pair = jnp.concatenate([u1 * w2 - u2 * w1, u2 * w0 - u0 * w2], 1)
    back_pair = right_apply(pair, forward_pair)
    back_one = right_apply(u0 * w1 - u1 * w0, forward_one)
    return left_apply(
        gather,
        jnp.concatenate(
            [
                jnp.concatenate([back_pair[:, :LANES], back_one[:, :LANES]], 1),
                jnp.concatenate([back_pair[:, LANES:], back_one[:, LANES:]], 1),
            ],
            0,
        ),
    )


def gather_waves(fetched, state, a, tables, gather):
    kxy, kz, inverse, damping = tables[0][a], tables[3][...], tables[4][a], tables[5][a]
    rows = [
        jnp.concatenate(
            [
                fetched[pl.ds(8 * g + LOCAL * h + a, G // 2, stride=B_ROWS), :]
                for h in range(2)
            ],
            0,
        )
        for g in range(2)
    ]
    turned = [turn(r) for r in rows]
    modes = left_apply(
        gather, jnp.concatenate([jnp.concatenate(rows, 1), jnp.concatenate(turned, 1)], 0)
    )
    first, third = modes[:, :LANES], modes[:, LANES:]
    along = kxy * first
    divergence = (along + pltpu.roll(along, PAIR, 1) + kz * third) * inverse
    return (
        damping * (state[a, :, :LANES] + time_step * (first - kxy * divergence)),
        damping * (state[a, :, LANES:] + time_step * (third - kz * divergence)),
    )


def chain_kernel(
    low, start, fine_end,
    kxy, ky, kzx, kz, inverse, damping,
    spread, gather, spread_rows, gather_rows, inverse_pair, forward_pair, forward_one,
    result, previous,
    states, terms, term,
    own_out_f, own_in_f, own_out_b, own_in_b, out_f, in_f, out_b, in_b,
    end_send, end_recv, term_send, term_recv, state_send, state_recv,
    own_f_send, own_f_recv, own_b_send, own_b_recv, f_send, f_recv, b_send, b_recv,
):
    mats = tuple(m[...] for m in (spread, gather, inverse_pair, forward_pair, forward_one))
    spread_x, gather_x = spread_rows[...], gather_rows[...]
    slot, py, pz = lax.axis_index("tm"), lax.axis_index("py"), lax.axis_index("pz")
    slices = lax.axis_size("tm")
    stride = slices // 4
    side = slot // stride
    is_chain = (pz == 0) & (slot % stride == 0)
    own_term = (slot == 0) & (pz == 0)
    sends_term = jnp.logical_not(own_term) & (slot < slices - 1)

    def tables_of(which):
        return (kxy.at[which], ky.at[which], kzx, kz, inverse.at[which], damping.at[which])

    def slice_device(peer):
        return (slot, peer // 4, peer % 4)

    def chain_device(peer):
        return (peer % 4 * stride, peer // 4, 0)

    def term_copy(source_slice):
        return pltpu.make_async_remote_copy(
            src_ref=term,
            dst_ref=terms.at[source_slice],
            send_sem=term_send,
            recv_sem=term_recv.at[source_slice],
            device_id=(pz * stride, py, 0),
            device_id_type=MESH,
        )

    def state_copy(t):
        return pltpu.make_async_remote_copy(
            src_ref=states.at[t],
            dst_ref=result,
            send_sem=state_send.at[t],
            recv_sem=state_recv,
            device_id=(t, py, side),
            device_id_type=MESH,
        )

    def advance_into(state, tables, me, device_of, buffers, sems, write):
        out_f, in_f, out_b, in_b = buffers
        f_send, f_recv, b_send, b_recv = sems

        def send(source, target, sends, recvs, rows, k):
            def piece(which):
                return pl.ds(pl.multiple_of((which * PIECES + k) * rows, 8), rows)

            def one(j, carried):
                peer = (me + j) % PARTS
                pltpu.make_async_remote_copy(
                    src_ref=source.at[piece(peer), :],
                    dst_ref=target.at[piece(me), :],
                    send_sem=sends.at[k],
                    recv_sem=recvs.at[k],
                    device_id=device_of(peer),
                    device_id_type=MESH,
                ).start()
                return carried

            lax.fori_loop(1, PARTS, one, 0)
            target[piece(me), :] = source[piece(me), :]

        def drain(buffer, sems, rows, k):
            bulk = buffer.at[pl.ds(0, rows * (PARTS - 1)), :]
            pltpu.make_async_copy(bulk, bulk, sems.at[k]).wait()

        forth = (out_f, in_f, f_send, f_recv, F_ROWS)
        back = (out_b, in_b, b_send, b_recv, B_ROWS)
        for a in range(LOCAL):
            waves = spread_waves(state, a, tables, spread_x)
            for g in range(3):
                for h in range(2):
                    out_f[pl.ds(8 * g + LOCAL * h + a, G // 2, stride=F_ROWS), :] = waves[
                        G // 2 * h : G // 2 * (h + 1), LANES * g : LANES * (g + 1)
                    ]
        for k in range(PIECES):
            send(*forth, k)
        for k in range(PIECES):
            drain(in_f, f_recv, F_ROWS, k)
            for x in (2 * k, 2 * k + 1):
                made = plane_product(in_f, x, mats)
                for g in range(2):
                    for a in range(LOCAL):
                        first_row = B_ROWS * k + 8 * g + LOCAL * (x % 2) + a
                        out_b[pl.ds(first_row, PARTS, stride=B_ROWS * PIECES), :] = made[
                            PARTS * a : PARTS * (a + 1), LANES * g : LANES * (g + 1)
                        ]
            send(*back, k)
        for k in range(PIECES):
            drain(out_f, f_send, F_ROWS, k)
        for k in range(PIECES):
            drain(in_b, b_recv, B_ROWS, k)
        for a in range(LOCAL):
            write(a, *gather_waves(in_b, state, a, tables, gather_x))
        for k in range(PIECES):
            drain(out_b, b_send, B_ROWS, k)

    end_copy = pltpu.make_async_remote_copy(
        src_ref=fine_end,
        dst_ref=previous,
        send_sem=end_send,
        recv_sem=end_recv,
        device_id=((slot + 1) % slices, py, pz),
        device_id_type=MESH,
    )

    def write_term(a, first, third):
        @pl.when(slot == 0)
        def _():
            term[a] = low[a]

        @pl.when(slot != 0)
        def _():
            term[a, :, :LANES] = low[a, :, :LANES] - first
            term[a, :, LANES:] = low[a, :, LANES:] - third

    advance_into(
        start,
        tables_of(0),
        py * 4 + pz,
        slice_device,
        (own_out_f, own_in_f, own_out_b, own_in_b),
        (own_f_send, own_f_recv, own_b_send, own_b_recv),
        write_term,
    )

    @pl.when(sends_term)
    def _():
        term_copy(slot).start()

    @pl.when(slot < slices - 1)
    def _():
        end_copy.start()

    @pl.when(slot == 0)
    def _():
        result[...] = jnp.zeros_like(result)

    @pl.when(is_chain)
    def _():
        @pl.when(own_term)
        def _():
            states[1] = term[...]

        @pl.when(jnp.logical_not(own_term))
        def _():
            term_copy(0).wait_recv()
            states[1] = terms[0]

        def step(t, carried):
            state_copy(t).start()

            def write_state(a, first, third):
                if a == 0:
                    term_copy(t).wait_recv()
                states[t + 1, a, :, :LANES] = first + terms[t, a, :, :LANES]
                states[t + 1, a, :, LANES:] = third + terms[t, a, :, LANES:]

            advance_into(
                states.at[t],
                tables_of(1),
                py * 4 + side,
                chain_device,
                (out_f, in_f, out_b, in_b),
                (f_send, f_recv, b_send, b_recv),
                write_state,
            )
            return carried

        lax.fori_loop(1, slices - 1, step, 0)
        state_copy(slices - 1).start()

        def finish_state(t, carried):
            state_copy(t).wait_send()
            return carried

        lax.fori_loop(1, slices, finish_state, 0)

    @pl.when(sends_term)
    def _():
        term_copy(slot).wait_send()

    @pl.when(slot < slices - 1)
    def _():
        end_copy.wait_send()

    @pl.when(slot != 0)
    def _():
        state_copy(slot).wait_recv()
        end_copy.wait_recv()


def half_turn(x):
    lane = lax.broadcasted_iota(jnp.int32, x.shape, 1)
    rolled = pltpu.roll(x, LANES // 2, 1)
    return jnp.where(lane < LANES // 2, -rolled, rolled)


def fine_kernel(
    start, spread, gather, inverse, forward,
    state, fine_end,
    out_f, in_f, out_b, in_b, f_send, f_recv, b_send, b_recv,
):
    slot, py, pz = lax.axis_index("tm"), lax.axis_index("py"), lax.axis_index("pz")
    me = py * 4 + pz
    modes = start.shape[1] // FINE_LOCAL
    planes = in_f.shape[0]
    extent = planes * PARTS
    shape = (modes, LANES)
    rows = lax.broadcasted_iota(jnp.int32, shape, 0)
    kx = jnp.where(rows < modes // 2, rows, rows - modes).astype(jnp.float32)
    kz = (lax.broadcasted_iota(jnp.int32, shape, 1) % (LANES // 2)).astype(jnp.float32)

    def wave_y(a):
        place = a * PARTS + me
        return jnp.where(place < modes // 2, place, place - modes).astype(jnp.float32)

    def without_divergence(fields, ky, squared):
        divergence = (kx * fields[0] + ky * fields[1] + kz * fields[2]) / jnp.maximum(squared, 1.0)
        return (
            fields[0] - kx * divergence,
            fields[1] - ky * divergence,
            fields[2] - kz * divergence,
        )

    for a in range(FINE_LOCAL):
        ky = wave_y(a)
        squared = kx * kx + ky * ky + kz * kz
        picked = pl.ds(a, modes, stride=FINE_LOCAL)
        fields = without_divergence([start[c, picked, :] for c in range(3)], ky, squared)
        for c in range(3):
            state[c, picked, :] = fields[c]
        turned = [half_turn(v) for v in fields]
        wide = jnp.concatenate([*fields, kx * fields[1], kx * fields[2]], 1)
        wide_turned = jnp.concatenate([*turned, kx * turned[1], kx * turned[2]], 1)
        waves = left_apply(spread[...], jnp.concatenate([wide, wide_turned], 0))
        for c in range(5):
            out_f[pl.ds(8 * c + a, extent, stride=FINE_F), :] = waves[:, LANES * c : LANES * (c + 1)]

    def device_of(peer):
        return (slot, peer // 4, peer % 4)

    def send_plane(x, carried):
        def one(j, carried):
            peer = (me + j) % PARTS
            first = pl.multiple_of((peer * planes + x) * FINE_F, 8)
            pltpu.make_async_remote_copy(
                src_ref=out_f.at[pl.ds(first, FINE_F), :],
                dst_ref=in_f.at[x, pl.ds(pl.multiple_of(me * FINE_F, 8), FINE_F), :],
                send_sem=f_send,
                recv_sem=f_recv.at[x],
                device_id=device_of(peer),
                device_id_type=MESH,
            ).start()
            return carried

        lax.fori_loop(1, PARTS, one, 0)
        mine = pl.multiple_of((me * planes + x) * FINE_F, 8)
        in_f[x, pl.ds(pl.multiple_of(me * FINE_F, 8), FINE_F), :] = out_f[pl.ds(mine, FINE_F), :]
        return carried

    lax.fori_loop(0, planes, send_plane, 0)
    places = lax.broadcasted_iota(jnp.int32, shape, 0)
    ky_rows = jnp.where(places < modes // 2, places, places - modes).astype(jnp.float32)

    def plane(x, carried):
        bulk = in_f.at[x, pl.ds(0, FINE_F * (PARTS - 1)), :]
        pltpu.make_async_copy(bulk, bulk, f_recv.at[x]).wait()
        arrived = [
            jnp.concatenate(
                [in_f[x, pl.ds(8 * c + a, PARTS, stride=FINE_F), :] for a in range(FINE_LOCAL)], 0
            )
            for c in range(5)
        ]
        raw = [
            ky_rows * arrived[2] - kz * arrived[1],
            kz * arrived[0] - arrived[4],
            arrived[3] - ky_rows * arrived[0],
        ]
        fields = jnp.concatenate(arrived[:3] + [half_turn(w) for w in raw], 1)
        turned = jnp.concatenate([half_turn(v) for v in arrived[:3]] + [-w for w in raw], 1)
        along_y = left_apply(spread[...], jnp.concatenate([fields, turned], 0))
        u0, u1, u2, w0, w1, w2 = [
            right_apply(along_y[:, LANES * c : LANES * (c + 1)], inverse[...]) for c in range(6)
        ]
        back = [
            right_apply(n, forward[...])
            for n in (u1 * w2 - u2 * w1, u2 * w0 - u0 * w2, u0 * w1 - u1 * w0)
        ]
        made = left_apply(
            gather[...],
            jnp.concatenate(
                [
                    jnp.concatenate([b[:, :LANES] for b in back], 1),
                    jnp.concatenate([b[:, LANES:] for b in back], 1),
                ],
                0,
            ),
        )
        for c in range(3):
            for a in range(FINE_LOCAL):
                out_b[x, pl.ds(8 * c + a, PARTS, stride=FINE_B), :] = made[
                    PARTS * a : PARTS * (a + 1), LANES * c : LANES * (c + 1)
                ]
        home = pl.ds(pl.multiple_of((me * planes + x) * FINE_B, 8), FINE_B)

        def one(j, carried):
            peer = (me + j) % PARTS
            pltpu.make_async_remote_copy(
                src_ref=out_b.at[x, pl.ds(pl.multiple_of(peer * FINE_B, 8), FINE_B), :],
                dst_ref=in_b.at[home, :],
                send_sem=b_send,
                recv_sem=b_recv,
                device_id=device_of(peer),
                device_id_type=MESH,
            ).start()
            return carried

        lax.fori_loop(1, PARTS, one, 0)
        in_b[home, :] = out_b[x, pl.ds(pl.multiple_of(me * FINE_B, 8), FINE_B), :]
        return carried

    lax.fori_loop(0, planes, plane, 0)
    sent = out_f.at[pl.ds(0, planes * (PARTS - 1) * FINE_F), :]
    pltpu.make_async_copy(sent, sent, f_send).wait()
    bulk = in_b.at[pl.ds(0, planes * (PARTS - 1) * FINE_B), :]
    pltpu.make_async_copy(bulk, bulk, b_recv).wait()
    for a in range(FINE_LOCAL):
        ky = wave_y(a)
        squared = kx * kx + ky * ky + kz * kz
        picked = pl.ds(a, modes, stride=FINE_LOCAL)
        columns = [in_b[pl.ds(8 * c + a, extent, stride=FINE_B), :] for c in range(3)]
        turned = [half_turn(v) for v in columns]
        narrow = left_apply(
            gather[...],
            jnp.concatenate([jnp.concatenate(columns, 1), jnp.concatenate(turned, 1)], 0),
        )
        pushed = without_divergence(
            [narrow[:, LANES * c : LANES * (c + 1)] for c in range(3)], ky, squared
        )
        damping = jnp.exp(-viscosity * time_step * squared)
        for c in range(3):
            fine_end[c, picked, :] = damping * (state[c, picked, :] + time_step * pushed[c])
    pltpu.make_async_copy(bulk, bulk, b_send).wait()


def fine_step(stored):
    retained = stored.shape[1]
    extent = 3 * retained // 2
    planes = extent // PARTS
    spread, gather = transform_pair(retained)
    inverse, forward, turned = depth_transforms(retained, 2 * LANES)
    operands = [
        stored.reshape(3, retained * FINE_LOCAL, LANES),
        stacked(spread, 1),
        stacked(gather, 1),
        stacked(inverse, 0),
        stacked(np.concatenate([forward, turned], 1), 0),
    ]
    vmem = pl.BlockSpec(memory_space=pltpu.VMEM)
    block = jax.ShapeDtypeStruct(operands[0].shape, jnp.float32)
    made = pl.pallas_call(
        fine_kernel,
        out_shape=(block, block),
        in_specs=[vmem] * len(operands),
        out_specs=(vmem, vmem),
        scratch_shapes=[
            pltpu.VMEM((extent * FINE_F, LANES), jnp.float32),
            pltpu.VMEM((planes, PARTS * FINE_F, LANES), jnp.float32),
            pltpu.VMEM((planes, PARTS * FINE_B, LANES), jnp.float32),
            pltpu.VMEM((extent * FINE_B, LANES), jnp.float32),
            pltpu.SemaphoreType.DMA,
            pltpu.SemaphoreType.DMA((planes,)),
            pltpu.SemaphoreType.DMA,
            pltpu.SemaphoreType.DMA,
        ],
        compiler_params=pltpu.CompilerParams(
            has_side_effects=True, vmem_limit_bytes=40 * 1024 * 1024
        ),
    )(*operands)
    return [one.reshape(stored.shape) for one in made]


def packed_coarse(coeffs):
    moved = coeffs.transpose(2, 1, 0, 3)
    doubled = jnp.concatenate([moved, moved[:, :, 2:]], axis=2)
    return doubled.reshape(LOCAL, M, 2 * LANES)


def chain(low, start, fine_end, member, slices):
    chain_member = lax.axis_index("py") * 4 + lax.axis_index("tm") // (slices // 4)
    own, chained = wave_tables(member), wave_tables(chain_member)
    stacked = [
        one if n in (2, 3) else jnp.stack([one, two])
        for n, (one, two) in enumerate(zip(own, chained))
    ]
    vmem = pl.BlockSpec(memory_space=pltpu.VMEM)
    operands = [packed_coarse(low), packed_coarse(start), fine_end, *stacked, *coarse_matrices()]
    block = (LOCAL, M, 2 * LANES)
    wide = pltpu.VMEM((PARTS * PIECES * F_ROWS, LANES), jnp.float32)
    narrow = pltpu.VMEM((PARTS * PIECES * B_ROWS, LANES), jnp.float32)
    pieces = pltpu.SemaphoreType.DMA((PIECES,))
    anywhere = pl.BlockSpec(memory_space=pl.ANY)
    made, previous = pl.pallas_call(
        chain_kernel,
        out_shape=(
            jax.ShapeDtypeStruct(block, jnp.float32),
            jax.ShapeDtypeStruct(fine_end.shape, jnp.float32),
        ),
        in_specs=[vmem, vmem, anywhere] + [vmem] * (len(operands) - 3),
        out_specs=(vmem, anywhere),
        scratch_shapes=[
            pltpu.VMEM((slices,) + block, jnp.float32),
            pltpu.VMEM((slices,) + block, jnp.float32),
            pltpu.VMEM(block, jnp.float32),
            wide, wide, narrow, narrow,
            wide, wide, narrow, narrow,
            pltpu.SemaphoreType.DMA,
            pltpu.SemaphoreType.DMA,
            pltpu.SemaphoreType.DMA,
            pltpu.SemaphoreType.DMA((slices,)),
            pltpu.SemaphoreType.DMA((slices,)),
            pltpu.SemaphoreType.DMA,
            pieces, pieces, pieces, pieces,
            pieces, pieces, pieces, pieces,
        ],
        cost_estimate=pl.CostEstimate(
            flops=10**11, bytes_accessed=10**7, transcendentals=0
        ),
        compiler_params=pltpu.CompilerParams(
            has_side_effects=True, vmem_limit_bytes=32 * 1024 * 1024
        ),
    )(*operands)
    return made.reshape(LOCAL, M, 4, PAIR)[:, :, :3].transpose(2, 1, 0, 3), previous


def shards(start_states):
    count_py = lax.axis_size("py")
    count_pz = lax.axis_size("pz")
    groups = count_py * count_pz
    member = lax.axis_index("py") * count_pz + lax.axis_index("pz")
    position = lax.axis_index("tm")
    slices = lax.axis_size("tm")
    retained = start_states.shape[-1]
    stored = start_states.reshape(3, retained, start_states.shape[3], retained)
    spectral_state, fine_end = fine_step(stored)
    coarse_start = restrict(spectral_state, M, groups)
    fine_low = restrict(fine_end, M, groups)
    current, previous = chain(fine_low, coarse_start, fine_end, member, slices)
    upper_band = previous - prolong(restrict(previous, M, groups), retained, groups)
    updated = prolong(current, retained, groups) + upper_band
    result = jnp.where(position == 0, spectral_state, updated)
    return result.reshape(1, result.shape[0], retained, result.shape[2], 1, retained)


def solution(mesh):
    in_specs = (P("tm", None, None, None, ("py", "pz"), None),)
    out_specs = P("tm", None, None, None, ("py", "pz"), None)
    return jax.shard_map(shards, mesh=mesh, in_specs=in_specs, out_specs=out_specs, check_vma=False)
```

```python
from functools import partial

import jax
import jax.numpy as jnp
from jax import lax
from jax.experimental import pallas as pl
from jax.experimental.pallas import tpu as pltpu
import numpy as np
from jax.sharding import PartitionSpec as P

M = 64


viscosity = 0.03
time_step = 0.004


G = 3 * M // 2
PARTS = 16
LOCAL = M // PARTS
PLANES = G // PARTS
PIECES = PLANES // 2
FINE_LOCAL = 8
FINE_F = 5 * FINE_LOCAL
FINE_B = 3 * FINE_LOCAL
F_ROWS = 24
B_ROWS = 16
LANES = 128
PAIR = LANES // 2
QUAD = PAIR // 2
MESH = pl.DeviceIdType.MESH


def halves(matrix):
    high = np.asarray(matrix, np.float32).astype(jnp.bfloat16)
    low = (np.asarray(matrix, np.float32) - high.astype(np.float32)).astype(jnp.bfloat16)
    return high, low


def stacked(matrix, axis):
    high, low = halves(matrix)
    return jnp.asarray(np.concatenate([high, high, low], axis))


def transform_pair(retained):
    extent = 3 * retained // 2
    points = np.arange(extent)
    waves = np.where(np.arange(retained) < retained // 2, np.arange(retained), np.arange(retained) - retained)
    angle = (points[:, None] * waves[None, :]) % extent * (2.0 * np.pi / extent)
    spread = np.concatenate([np.cos(angle), np.sin(angle)], 1) * retained**-0.5
    gather = np.concatenate([np.cos(angle.T), -np.sin(angle.T)], 1) * (retained**0.5 / extent)
    return spread, gather


def depth_transforms(retained, lanes):
    extent, half = 3 * retained // 2, retained // 2
    points, harmonic = np.arange(extent), np.arange(half)
    angle = (points[:, None] * harmonic[None, :]) % extent * (2.0 * np.pi / extent)
    weight = np.where(harmonic == 0, 1.0, 2.0) * retained**-0.5
    inverse = np.zeros((retained, lanes))
    inverse[:, :extent] = np.concatenate([np.cos(angle) * weight, -np.sin(angle) * weight], 1).T
    forward = np.zeros((lanes, retained))
    forward[:extent] = np.concatenate([np.cos(angle), -np.sin(angle)], 1) * (retained**0.5 / extent)
    turned = np.concatenate([-forward[:, half:], forward[:, :half]], 1)
    return inverse, forward, turned


def transforms(retained):
    spread, gather = transform_pair(M)
    inverse, forward, turned = depth_transforms(M, LANES)
    none_in = np.zeros_like(inverse)
    none_out = np.zeros_like(forward)
    inverse_pair = np.block([[inverse, none_in], [none_in, inverse]])
    forward_pair = np.block(
        [[forward, none_out, turned, none_out], [none_out, forward, none_out, turned]]
    )
    forward_one = np.concatenate([forward, forward, turned, turned], 1)
    order = np.concatenate([np.arange(0, G, 2), np.arange(1, G, 2)])
    gather_rows = np.concatenate([gather[:, order], gather[:, G + order]], 1)
    fine_spread, fine_gather = transform_pair(retained)
    fine_inverse, fine_forward, fine_turned = depth_transforms(retained, 2 * LANES)
    fine_back = np.concatenate([fine_forward, fine_turned], 1)
    deep = [stacked(m, 0) for m in (fine_inverse, fine_back, inverse_pair, forward_pair, forward_one)]
    edges = np.cumsum([0] + [m.shape[0] for m in deep]).tolist()
    operands = [
        stacked(fine_spread, 1),
        stacked(fine_gather, 1),
        jnp.concatenate(deep, 0),
        jnp.concatenate([stacked(spread, 1), stacked(spread[order], 1)], 0),
        jnp.concatenate([stacked(gather, 1), stacked(gather_rows, 1)], 0),
    ]
    return operands, edges


def turn(x):
    lane = lax.broadcasted_iota(jnp.int32, x.shape, 1)
    return jnp.where(
        lane % PAIR < QUAD, -pltpu.roll(x, LANES - QUAD, 1), pltpu.roll(x, QUAD, 1)
    )


def split(x):
    high = x.astype(jnp.bfloat16)
    return high, (x - high.astype(jnp.float32)).astype(jnp.bfloat16)


def left_apply(matrix, x):
    high, low = split(x)
    return jnp.dot(
        matrix, jnp.concatenate([high, low, high], 0), preferred_element_type=jnp.float32
    )


def right_apply(x, matrix):
    high, low = split(x)
    return jnp.dot(
        jnp.concatenate([high, low, high], 1), matrix, preferred_element_type=jnp.float32
    )


def spread_waves(state, a, tables, spread):
    kx, ky, kz = tables[0], tables[1](a), tables[2]
    first, third = state[a, :, :LANES], state[a, :, LANES:]
    lower = lax.broadcasted_iota(jnp.int32, first.shape, 1) < PAIR
    kxy, kzx = jnp.where(lower, kx, ky), jnp.where(lower, kz, kx)
    raw_one = ky * third - kz * first
    raw_two = kzx * first - kxy * jnp.where(lower, third, pltpu.roll(first, PAIR, 1))
    fields = jnp.concatenate(
        [first, jnp.where(lower, third, turn(raw_one)), turn(raw_two)], 1
    )
    turned = jnp.concatenate(
        [turn(first), jnp.where(lower, turn(third), -raw_one), -raw_two], 1
    )
    return left_apply(spread, jnp.concatenate([fields, turned], 0))


def plane_product(fetched, x, mats):
    spread, gather, inverse_pair, forward_pair, forward_one = mats
    fields, turned = [], []
    for g in range(3):
        rows = jnp.concatenate(
            [
                fetched[
                    pl.ds(
                        F_ROWS * (x // 2) + 8 * g + LOCAL * (x % 2) + a,
                        PARTS,
                        stride=F_ROWS * PIECES,
                    ),
                    :,
                ]
                for a in range(LOCAL)
            ],
            0,
        )
        fields.append(rows)
        turned.append(turn(rows))
    along_y = left_apply(
        spread, jnp.concatenate([jnp.concatenate(fields, 1), jnp.concatenate(turned, 1)], 0)
    )
    grids = [
        right_apply(along_y[:, LANES * g : LANES * (g + 1)], inverse_pair) for g in range(3)
    ]
    u0, u1 = grids[0][:, :LANES], grids[0][:, LANES:]
    u2, w0 = grids[1][:, :LANES], grids[1][:, LANES:]
    w1, w2 = grids[2][:, :LANES], grids[2][:, LANES:]
    pair = jnp.concatenate([u1 * w2 - u2 * w1, u2 * w0 - u0 * w2], 1)
    back_pair = right_apply(pair, forward_pair)
    back_one = right_apply(u0 * w1 - u1 * w0, forward_one)
    return left_apply(
        gather,
        jnp.concatenate(
            [
                jnp.concatenate([back_pair[:, :LANES], back_one[:, :LANES]], 1),
                jnp.concatenate([back_pair[:, LANES:], back_one[:, LANES:]], 1),
            ],
            0,
        ),
    )


def gather_waves(fetched, state, a, tables, gather):
    kx, ky, kz, inverse, damping = tables[0], tables[1](a), tables[2], tables[3][a], tables[4][a]
    kxy = jnp.where(lax.broadcasted_iota(jnp.int32, kx.shape, 1) < PAIR, kx, ky)
    rows = [
        jnp.concatenate(
            [
                fetched[pl.ds(8 * g + LOCAL * h + a, G // 2, stride=B_ROWS), :]
                for h in range(2)
            ],
            0,
        )
        for g in range(2)
    ]
    turned = [turn(r) for r in rows]
    modes = left_apply(
        gather, jnp.concatenate([jnp.concatenate(rows, 1), jnp.concatenate(turned, 1)], 0)
    )
    first, third = modes[:, :LANES], modes[:, LANES:]
    along = kxy * first
    divergence = (along + pltpu.roll(along, PAIR, 1) + kz * third) * inverse
    return (
        damping * (state[a, :, :LANES] + time_step * (first - kxy * divergence)),
        damping * (state[a, :, LANES:] + time_step * (third - kz * divergence)),
    )


def half_turn(x):
    lane = lax.broadcasted_iota(jnp.int32, x.shape, 1)
    rolled = pltpu.roll(x, LANES // 2, 1)
    return jnp.where(lane < LANES // 2, -rolled, rolled)


def pack_pair(first, second):
    lane = lax.broadcasted_iota(jnp.int32, first.shape, 1)
    lower = jnp.where(lane < QUAD, first, pltpu.roll(first, LANES - QUAD, 1))
    upper = jnp.where(lane < LANES - QUAD, pltpu.roll(second, PAIR, 1), pltpu.roll(second, QUAD, 1))
    return jnp.where(lane < PAIR, lower, upper)


def kept_rows(x):
    return jnp.concatenate([x[: M // 2], x[x.shape[0] - M // 2 :]], 0)


def iteration_kernel(
    edges,
    start, fine_spread, fine_gather, deep, coarse_spread, coarse_gather,
    result,
    state, fine_end, fine_out_f, fine_in_f, fine_out_b, fine_in_b,
    coarse_start, inverses, dampings, states, terms, term, landed,
    own_out_f, own_in_f, own_out_b, own_in_b, out_f, in_f, out_b, in_b,
    fine_f_send, fine_f_recv, fine_b_send, fine_b_recv,
    end_send, end_recv, term_send, term_recv, state_send, state_recv,
    own_f_send, own_f_recv, own_b_send, own_b_recv, f_send, f_recv, b_send, b_recv,
):
    slot, py, pz = lax.axis_index("tm"), lax.axis_index("py"), lax.axis_index("pz")
    slices = lax.axis_size("tm")
    stride = slices // 4
    side = slot // stride
    me = py * 4 + pz
    is_chain = (pz == 0) & (slot % stride == 0)
    own_term = (slot == 0) & (pz == 0)
    sends_term = jnp.logical_not(own_term) & (slot < slices - 1)
    fine_inverse, fine_back, inverse_pair, forward_pair, forward_one = [
        deep.at[pl.ds(low, high - low), :] for low, high in zip(edges, edges[1:])
    ]
    points, kept = G, M
    mats = (
        coarse_spread[:points], coarse_gather[:kept],
        inverse_pair[...], forward_pair[...], forward_one[...],
    )
    spread_x, gather_x = coarse_spread[points:], coarse_gather[kept:]

    def place_wave(place, length):
        return jnp.where(place < length // 2, place, place - length).astype(jnp.float32)

    coarse_shape = (M, LANES)
    coarse_kx = place_wave(lax.broadcasted_iota(jnp.int32, coarse_shape, 0), M)
    coarse_kz = (lax.broadcasted_iota(jnp.int32, coarse_shape, 1) % QUAD).astype(jnp.float32)
    members = (me, py * 4 + side)

    def coarse_ky(which):
        return lambda a: place_wave(a * PARTS + members[which], M)

    def tables_of(which):
        return (coarse_kx, coarse_ky(which), coarse_kz, inverses.at[which], dampings.at[which])

    for which in range(2):
        for a in range(LOCAL):
            ky = coarse_ky(which)(a)
            squared = coarse_kx * coarse_kx + ky * ky + coarse_kz * coarse_kz
            inverses[which, a] = 1.0 / jnp.maximum(squared, 1.0)
            dampings[which, a] = jnp.exp(-viscosity * time_step * squared)

    def slice_device(peer):
        return (slot, peer // 4, peer % 4)

    def chain_device(peer):
        return (peer % 4 * stride, peer // 4, 0)

    def for_peers(who, act):
        def some(i, carried):
            for u in range(5):
                act((who + 1 + 5 * i + u) % PARTS)
            return carried

        lax.fori_loop(0, 3, some, 0)

    def term_copy(source_slice):
        return pltpu.make_async_remote_copy(
            src_ref=term,
            dst_ref=terms.at[source_slice],
            send_sem=term_send,
            recv_sem=term_recv.at[source_slice],
            device_id=(pz * stride, py, 0),
            device_id_type=MESH,
        )

    def state_copy(t):
        return pltpu.make_async_remote_copy(
            src_ref=states.at[t],
            dst_ref=landed,
            send_sem=state_send.at[t],
            recv_sem=state_recv,
            device_id=(t, py, side),
            device_id_type=MESH,
        )

    def advance_parts(state, tables, me, device_of, buffers, sems, write):
        out_f, in_f, out_b, in_b = buffers
        f_send, f_recv, b_send, b_recv = sems

        def send(source, target, sends, recvs, rows, k):
            def piece(which):
                return pl.ds(pl.multiple_of((which * PIECES + k) * rows, 8), rows)

            def one(peer):
                pltpu.make_async_remote_copy(
                    src_ref=source.at[piece(peer), :],
                    dst_ref=target.at[piece(me), :],
                    send_sem=sends.at[k],
                    recv_sem=recvs.at[k],
                    device_id=device_of(peer),
                    device_id_type=MESH,
                ).start()

            for_peers(me, one)
            target[piece(me), :] = source[piece(me), :]

        def drain(buffer, sems, rows, k):
            bulk = buffer.at[pl.ds(0, rows * (PARTS - 1)), :]
            pltpu.make_async_copy(bulk, bulk, sems.at[k]).wait()

        forth = (out_f, in_f, f_send, f_recv, F_ROWS)
        back = (out_b, in_b, b_send, b_recv, B_ROWS)
        def begin():
            for a in range(LOCAL):
                waves = spread_waves(state, a, tables, spread_x)
                for g in range(3):
                    for h in range(2):
                        out_f[pl.ds(8 * g + LOCAL * h + a, G // 2, stride=F_ROWS), :] = waves[
                            G // 2 * h : G // 2 * (h + 1), LANES * g : LANES * (g + 1)
                        ]
            for k in range(PIECES):
                send(*forth, k)

        def middle():
            for k in range(PIECES):
                drain(in_f, f_recv, F_ROWS, k)
                for x in (2 * k, 2 * k + 1):
                    made = plane_product(in_f, x, mats)
                    for g in range(2):
                        for a in range(LOCAL):
                            first_row = B_ROWS * k + 8 * g + LOCAL * (x % 2) + a
                            out_b[pl.ds(first_row, PARTS, stride=B_ROWS * PIECES), :] = made[
                                PARTS * a : PARTS * (a + 1), LANES * g : LANES * (g + 1)
                            ]
                send(*back, k)

        def end():
            for k in range(PIECES):
                drain(out_f, f_send, F_ROWS, k)
            for k in range(PIECES):
                drain(in_b, b_recv, B_ROWS, k)
            for a in range(LOCAL):
                write(a, *gather_waves(in_b, state, a, tables, gather_x))
            for k in range(PIECES):
                drain(out_b, b_send, B_ROWS, k)

        return begin, middle, end

    def write_own(a, first, third):
        term[a, :, :LANES] = first
        term[a, :, LANES:] = third

    own_begin, own_middle, own_end = advance_parts(
        coarse_start,
        tables_of(0),
        me,
        slice_device,
        (own_out_f, own_in_f, own_out_b, own_in_b),
        (own_f_send, own_f_recv, own_b_send, own_b_recv),
        write_own,
    )

    modes = start.shape[1] // FINE_LOCAL
    planes = fine_in_f.shape[0]
    extent = planes * PARTS
    shape = (modes, LANES)
    rows = lax.broadcasted_iota(jnp.int32, shape, 0)
    kx = jnp.where(rows < modes // 2, rows, rows - modes).astype(jnp.float32)
    kz = (lax.broadcasted_iota(jnp.int32, shape, 1) % (LANES // 2)).astype(jnp.float32)

    def wave_y(a):
        place = a * PARTS + me
        return jnp.where(place < modes // 2, place, place - modes).astype(jnp.float32)

    def without_divergence(fields, ky, squared):
        divergence = (kx * fields[0] + ky * fields[1] + kz * fields[2]) / jnp.maximum(squared, 1.0)
        return (
            fields[0] - kx * divergence,
            fields[1] - ky * divergence,
            fields[2] - kz * divergence,
        )

    kept_places = (*range(LOCAL // 2), *range(FINE_LOCAL - LOCAL // 2, FINE_LOCAL))
    for a in range(FINE_LOCAL):
        ky = wave_y(a)
        squared = kx * kx + ky * ky + kz * kz
        picked = pl.ds(a, modes, stride=FINE_LOCAL)
        fields = without_divergence([start[c, picked, :] for c in range(3)], ky, squared)
        for c in range(3):
            state[c, picked, :] = fields[c]
        if a in kept_places:
            slim = [kept_rows(v) for v in fields]
            coarse_start[kept_places.index(a), :, :LANES] = pack_pair(slim[0], slim[1])
            coarse_start[kept_places.index(a), :, LANES:] = pack_pair(slim[2], slim[2])
        turned = [half_turn(v) for v in fields]
        wide = jnp.concatenate([*fields, kx * fields[1], kx * fields[2]], 1)
        wide_turned = jnp.concatenate([*turned, kx * turned[1], kx * turned[2]], 1)
        waves = left_apply(fine_spread[...], jnp.concatenate([wide, wide_turned], 0))
        for c in range(5):
            fine_out_f[pl.ds(8 * c + a, extent, stride=FINE_F), :] = waves[:, LANES * c : LANES * (c + 1)]

    def send_plane(x, carried):
        def one(peer):
            first = pl.multiple_of((peer * planes + x) * FINE_F, 8)
            pltpu.make_async_remote_copy(
                src_ref=fine_out_f.at[pl.ds(first, FINE_F), :],
                dst_ref=fine_in_f.at[x, pl.ds(pl.multiple_of(me * FINE_F, 8), FINE_F), :],
                send_sem=fine_f_send,
                recv_sem=fine_f_recv.at[x],
                device_id=slice_device(peer),
                device_id_type=MESH,
            ).start()

        for_peers(me, one)
        mine = pl.multiple_of((me * planes + x) * FINE_F, 8)
        fine_in_f[x, pl.ds(pl.multiple_of(me * FINE_F, 8), FINE_F), :] = fine_out_f[pl.ds(mine, FINE_F), :]
        return carried

    own_begin()
    lax.fori_loop(0, planes, send_plane, 0)
    own_middle()
    places = lax.broadcasted_iota(jnp.int32, shape, 0)
    ky_rows = jnp.where(places < modes // 2, places, places - modes).astype(jnp.float32)

    def plane(x, carried):
        bulk = fine_in_f.at[x, pl.ds(0, FINE_F * (PARTS - 1)), :]
        pltpu.make_async_copy(bulk, bulk, fine_f_recv.at[x]).wait()
        arrived = [
            jnp.concatenate(
                [fine_in_f[x, pl.ds(8 * c + a, PARTS, stride=FINE_F), :] for a in range(FINE_LOCAL)], 0
            )
            for c in range(5)
        ]
        raw = [
            ky_rows * arrived[2] - kz * arrived[1],
            kz * arrived[0] - arrived[4],
            arrived[3] - ky_rows * arrived[0],
        ]
        fields = jnp.concatenate(arrived[:3] + [half_turn(w) for w in raw], 1)
        turned = jnp.concatenate([half_turn(v) for v in arrived[:3]] + [-w for w in raw], 1)
        along_y = left_apply(fine_spread[...], jnp.concatenate([fields, turned], 0))
        u0, u1, u2, w0, w1, w2 = [
            right_apply(along_y[:, LANES * c : LANES * (c + 1)], fine_inverse[...]) for c in range(6)
        ]
        back = [
            right_apply(n, fine_back[...])
            for n in (u1 * w2 - u2 * w1, u2 * w0 - u0 * w2, u0 * w1 - u1 * w0)
        ]
        made = left_apply(
            fine_gather[...],
            jnp.concatenate(
                [
                    jnp.concatenate([b[:, :LANES] for b in back], 1),
                    jnp.concatenate([b[:, LANES:] for b in back], 1),
                ],
                0,
            ),
        )
        for c in range(3):
            for a in range(FINE_LOCAL):
                fine_out_b[x, pl.ds(8 * c + a, PARTS, stride=FINE_B), :] = made[
                    PARTS * a : PARTS * (a + 1), LANES * c : LANES * (c + 1)
                ]
        home = pl.ds(pl.multiple_of((me * planes + x) * FINE_B, 8), FINE_B)

        def one(peer):
            pltpu.make_async_remote_copy(
                src_ref=fine_out_b.at[x, pl.ds(pl.multiple_of(peer * FINE_B, 8), FINE_B), :],
                dst_ref=fine_in_b.at[home, :],
                send_sem=fine_b_send,
                recv_sem=fine_b_recv,
                device_id=slice_device(peer),
                device_id_type=MESH,
            ).start()

        for_peers(me, one)
        fine_in_b[home, :] = fine_out_b[x, pl.ds(pl.multiple_of(me * FINE_B, 8), FINE_B), :]
        return carried

    lax.fori_loop(0, planes, plane, 0)
    own_end()
    sent = fine_out_f.at[pl.ds(0, planes * (PARTS - 1) * FINE_F), :]
    pltpu.make_async_copy(sent, sent, fine_f_send).wait()
    bulk = fine_in_b.at[pl.ds(0, planes * (PARTS - 1) * FINE_B), :]
    pltpu.make_async_copy(bulk, bulk, fine_b_recv).wait()
    for a in range(FINE_LOCAL):
        ky = wave_y(a)
        squared = kx * kx + ky * ky + kz * kz
        picked = pl.ds(a, modes, stride=FINE_LOCAL)
        columns = [fine_in_b[pl.ds(8 * c + a, extent, stride=FINE_B), :] for c in range(3)]
        turned = [half_turn(v) for v in columns]
        narrow = left_apply(
            fine_gather[...],
            jnp.concatenate([jnp.concatenate(columns, 1), jnp.concatenate(turned, 1)], 0),
        )
        pushed = without_divergence(
            [narrow[:, LANES * c : LANES * (c + 1)] for c in range(3)], ky, squared
        )
        damping = jnp.exp(-viscosity * time_step * squared)
        ends = [damping * (state[c, picked, :] + time_step * pushed[c]) for c in range(3)]
        for c in range(3):
            fine_end[c, picked, :] = ends[c]
        if a in kept_places:
            place = kept_places.index(a)
            slim = [kept_rows(v) for v in ends]
            for half, low in ((0, pack_pair(slim[0], slim[1])), (LANES, pack_pair(slim[2], slim[2]))):
                lanes = pl.ds(half, LANES)
                term[place, :, lanes] = low - jnp.where(slot == 0, 0.0, term[place, :, lanes])
    pltpu.make_async_copy(bulk, bulk, fine_b_send).wait()

    end_copy = pltpu.make_async_remote_copy(
        src_ref=fine_end,
        dst_ref=result,
        send_sem=end_send,
        recv_sem=end_recv,
        device_id=((slot + 1) % slices, py, pz),
        device_id_type=MESH,
    )

    @pl.when(sends_term)
    def _():
        term_copy(slot).start()

    @pl.when(slot < slices - 1)
    def _():
        end_copy.start()

    @pl.when(is_chain)
    def _():
        @pl.when(own_term)
        def _():
            states[1] = term[...]

        @pl.when(jnp.logical_not(own_term))
        def _():
            term_copy(0).wait_recv()
            states[1] = terms[0]

        def step(t, carried):
            state_copy(t).start()

            def write_state(a, first, third):
                if a == 0:
                    term_copy(t).wait_recv()
                states[t + 1, a, :, :LANES] = first + terms[t, a, :, :LANES]
                states[t + 1, a, :, LANES:] = third + terms[t, a, :, LANES:]

            begin, middle, end = advance_parts(
                states.at[t],
                tables_of(1),
                members[1],
                chain_device,
                (out_f, in_f, out_b, in_b),
                (f_send, f_recv, b_send, b_recv),
                write_state,
            )
            begin()
            middle()
            end()
            return carried

        lax.fori_loop(1, slices - 1, step, 0)
        state_copy(slices - 1).start()

        def finish_state(t, carried):
            state_copy(t).wait_send()
            return carried

        lax.fori_loop(1, slices, finish_state, 0)

    @pl.when(sends_term)
    def _():
        term_copy(slot).wait_send()

    @pl.when(slot < slices - 1)
    def _():
        end_copy.wait_send()

    @pl.when(slot == 0)
    def _():
        result[...] = state[...]

    @pl.when(slot != 0)
    def _():
        state_copy(slot).wait_recv()
        end_copy.wait_recv()
        half = M // 2
        lane = lax.broadcasted_iota(jnp.int32, (half, LANES), 1)
        real, imaginary = lane < QUAD, (lane >= PAIR) & (lane < PAIR + QUAD)
        for place, a in enumerate(kept_places):
            for top, first in ((0, 0), (half, modes - half)):
                pair = landed[place, pl.ds(top, half), :LANES]
                single = landed[place, pl.ds(top, half), LANES:]
                moved = (
                    (pair, pltpu.roll(pair, QUAD, 1)),
                    (pltpu.roll(pair, PAIR, 1), pltpu.roll(pair, LANES - QUAD, 1)),
                    (single, pltpu.roll(single, QUAD, 1)),
                )
                rows = pl.ds(first * FINE_LOCAL + a, half, stride=FINE_LOCAL)
                for c in range(3):
                    result[c, rows, :] = jnp.where(
                        real, moved[c][0], jnp.where(imaginary, moved[c][1], result[c, rows, :])
                    )


def shards(start_states):
    retained = start_states.shape[-1]
    extent = 3 * retained // 2
    planes = extent // PARTS
    slices = lax.axis_size("tm")
    matrices, edges = transforms(retained)
    operands = [start_states.reshape(3, retained * FINE_LOCAL, LANES), *matrices]
    vmem = pl.BlockSpec(memory_space=pltpu.VMEM)

    def floats(*shape):
        return pltpu.VMEM(shape, jnp.float32)

    block = (LOCAL, M, 2 * LANES)
    wide = floats(PARTS * PIECES * F_ROWS, LANES)
    narrow = floats(PARTS * PIECES * B_ROWS, LANES)
    single = pltpu.SemaphoreType.DMA
    pieces = pltpu.SemaphoreType.DMA((PIECES,))
    each = pltpu.SemaphoreType.DMA((slices,))
    result = pl.pallas_call(
        partial(iteration_kernel, edges),
        out_shape=jax.ShapeDtypeStruct(operands[0].shape, jnp.float32),
        in_specs=[vmem] * len(operands),
        out_specs=vmem,
        scratch_shapes=[
            floats(*operands[0].shape), floats(*operands[0].shape),
            floats(extent * FINE_F, LANES), floats(planes, PARTS * FINE_F, LANES),
            floats(planes, PARTS * FINE_B, LANES), floats(extent * FINE_B, LANES),
            floats(*block), floats(2, LOCAL, M, LANES), floats(2, LOCAL, M, LANES),
            floats(slices, *block), floats(slices, *block), floats(*block), floats(*block),
            wide, wide, narrow, narrow, wide, wide, narrow, narrow,
            single, pltpu.SemaphoreType.DMA((planes,)), single, single,
            single, single, single, each, each, single,
            pieces, pieces, pieces, pieces, pieces, pieces, pieces, pieces,
        ],
        compiler_params=pltpu.CompilerParams(
            has_side_effects=True, vmem_limit_bytes=56 * 1024 * 1024
        ),
    )(*operands)
    return result.reshape(start_states.shape)


def solution(mesh):
    in_specs = (P("tm", None, None, None, ("py", "pz"), None),)
    out_specs = P("tm", None, None, None, ("py", "pz"), None)
    return jax.shard_map(shards, mesh=mesh, in_specs=in_specs, out_specs=out_specs, check_vma=False)
```

```python
from functools import partial

import jax
import jax.numpy as jnp
from jax import lax
from jax.experimental import pallas as pl
from jax.experimental.pallas import tpu as pltpu
import numpy as np
from jax.sharding import PartitionSpec as P

M = 64


viscosity = 0.03
time_step = 0.004


G = 3 * M // 2
PARTS = 16
LOCAL = M // PARTS
PLANES = G // PARTS
PIECES = PLANES // 2
FINE_LOCAL = 8
FINE_F = 5 * FINE_LOCAL
FINE_B = 3 * FINE_LOCAL
F_ROWS = 24
B_ROWS = 16
LANES = 128
PAIR = LANES // 2
QUAD = PAIR // 2
MESH = pl.DeviceIdType.MESH


def halves(matrix):
    high = np.asarray(matrix, np.float32).astype(jnp.bfloat16)
    low = (np.asarray(matrix, np.float32) - high.astype(np.float32)).astype(jnp.bfloat16)
    return high, low


def stacked(matrix, axis):
    high, low = halves(matrix)
    return jnp.asarray(np.concatenate([high, high, low], axis))


def transform_pair(retained):
    extent = 3 * retained // 2
    points = np.arange(extent)
    waves = np.where(np.arange(retained) < retained // 2, np.arange(retained), np.arange(retained) - retained)
    angle = (points[:, None] * waves[None, :]) % extent * (2.0 * np.pi / extent)
    spread = np.concatenate([np.cos(angle), np.sin(angle)], 1) * retained**-0.5
    gather = np.concatenate([np.cos(angle.T), -np.sin(angle.T)], 1) * (retained**0.5 / extent)
    return spread, gather


def depth_transforms(retained, lanes):
    extent, half = 3 * retained // 2, retained // 2
    points, harmonic = np.arange(extent), np.arange(half)
    angle = (points[:, None] * harmonic[None, :]) % extent * (2.0 * np.pi / extent)
    weight = np.where(harmonic == 0, 1.0, 2.0) * retained**-0.5
    inverse = np.zeros((retained, lanes))
    inverse[:, :extent] = np.concatenate([np.cos(angle) * weight, -np.sin(angle) * weight], 1).T
    forward = np.zeros((lanes, retained))
    forward[:extent] = np.concatenate([np.cos(angle), -np.sin(angle)], 1) * (retained**0.5 / extent)
    turned = np.concatenate([-forward[:, half:], forward[:, :half]], 1)
    return inverse, forward, turned


def transforms(retained):
    spread, gather = transform_pair(M)
    inverse, forward, turned = depth_transforms(M, LANES)
    none_in = np.zeros_like(inverse)
    none_out = np.zeros_like(forward)
    inverse_pair = np.block([[inverse, none_in], [none_in, inverse]])
    forward_pair = np.block(
        [[forward, none_out, turned, none_out], [none_out, forward, none_out, turned]]
    )
    forward_one = np.concatenate([forward, forward, turned, turned], 1)
    order = np.concatenate([np.arange(0, G, 2), np.arange(1, G, 2)])
    gather_rows = np.concatenate([gather[:, order], gather[:, G + order]], 1)
    fine_spread, fine_gather = transform_pair(retained)
    fine_inverse, fine_forward, fine_turned = depth_transforms(retained, 2 * LANES)
    fine_back = np.concatenate([fine_forward, fine_turned], 1)
    deep = [stacked(m, 0) for m in (fine_inverse, fine_back, inverse_pair, forward_pair, forward_one)]
    edges = np.cumsum([0] + [m.shape[0] for m in deep]).tolist()
    operands = [
        stacked(fine_spread, 1),
        stacked(fine_gather, 1),
        jnp.concatenate(deep, 0),
        jnp.concatenate([stacked(spread, 1), stacked(spread[order], 1)], 0),
        jnp.concatenate([stacked(gather, 1), stacked(gather_rows, 1)], 0),
    ]
    return operands, edges


def turn(x):
    lane = lax.broadcasted_iota(jnp.int32, x.shape, 1)
    return jnp.where(
        lane % PAIR < QUAD, -pltpu.roll(x, LANES - QUAD, 1), pltpu.roll(x, QUAD, 1)
    )


def split(x):
    high = x.astype(jnp.bfloat16)
    return high, (x - high.astype(jnp.float32)).astype(jnp.bfloat16)


def left_apply(matrix, x):
    high, low = split(x)
    return jnp.dot(
        matrix, jnp.concatenate([high, low, high], 0), preferred_element_type=jnp.float32
    )


def right_apply(x, matrix):
    high, low = split(x)
    return jnp.dot(
        jnp.concatenate([high, low, high], 1), matrix, preferred_element_type=jnp.float32
    )


def spread_waves(state, a, tables, spread):
    kx, ky, kz = tables[0], tables[1](a), tables[2]
    first, third = state[a, :, :LANES], state[a, :, LANES:]
    lower = lax.broadcasted_iota(jnp.int32, first.shape, 1) < PAIR
    kxy, kzx = jnp.where(lower, kx, ky), jnp.where(lower, kz, kx)
    raw_one = ky * third - kz * first
    raw_two = kzx * first - kxy * jnp.where(lower, third, pltpu.roll(first, PAIR, 1))
    fields = jnp.concatenate(
        [first, jnp.where(lower, third, turn(raw_one)), turn(raw_two)], 1
    )
    turned = jnp.concatenate(
        [turn(first), jnp.where(lower, turn(third), -raw_one), -raw_two], 1
    )
    return left_apply(spread, jnp.concatenate([fields, turned], 0))


def plane_product(fetched, k, h, mats):
    spread, gather, inverse_pair, forward_pair, forward_one = mats
    fields, turned = [], []
    for g in range(3):
        rows = jnp.concatenate(
            [
                fetched[
                    pl.ds(
                        F_ROWS * k + 8 * g + LOCAL * h + a,
                        PARTS,
                        stride=F_ROWS * PIECES,
                    ),
                    :,
                ]
                for a in range(LOCAL)
            ],
            0,
        )
        fields.append(rows)
        turned.append(turn(rows))
    along_y = left_apply(
        spread, jnp.concatenate([jnp.concatenate(fields, 1), jnp.concatenate(turned, 1)], 0)
    )
    grids = [
        right_apply(along_y[:, LANES * g : LANES * (g + 1)], inverse_pair) for g in range(3)
    ]
    u0, u1 = grids[0][:, :LANES], grids[0][:, LANES:]
    u2, w0 = grids[1][:, :LANES], grids[1][:, LANES:]
    w1, w2 = grids[2][:, :LANES], grids[2][:, LANES:]
    pair = jnp.concatenate([u1 * w2 - u2 * w1, u2 * w0 - u0 * w2], 1)
    back_pair = right_apply(pair, forward_pair)
    back_one = right_apply(u0 * w1 - u1 * w0, forward_one)
    return left_apply(
        gather,
        jnp.concatenate(
            [
                jnp.concatenate([back_pair[:, :LANES], back_one[:, :LANES]], 1),
                jnp.concatenate([back_pair[:, LANES:], back_one[:, LANES:]], 1),
            ],
            0,
        ),
    )


def gather_waves(fetched, state, a, tables, gather):
    kx, ky, kz, inverse, damping = tables[0], tables[1](a), tables[2], tables[3][a], tables[4][a]
    kxy = jnp.where(lax.broadcasted_iota(jnp.int32, kx.shape, 1) < PAIR, kx, ky)
    rows = [
        jnp.concatenate(
            [
                fetched[pl.ds(8 * g + LOCAL * h + a, G // 2, stride=B_ROWS), :]
                for h in range(2)
            ],
            0,
        )
        for g in range(2)
    ]
    turned = [turn(r) for r in rows]
    modes = left_apply(
        gather, jnp.concatenate([jnp.concatenate(rows, 1), jnp.concatenate(turned, 1)], 0)
    )
    first, third = modes[:, :LANES], modes[:, LANES:]
    along = kxy * first
    divergence = (along + pltpu.roll(along, PAIR, 1) + kz * third) * inverse
    return (
        damping * (state[a, :, :LANES] + time_step * (first - kxy * divergence)),
        damping * (state[a, :, LANES:] + time_step * (third - kz * divergence)),
    )


def half_turn(x):
    lane = lax.broadcasted_iota(jnp.int32, x.shape, 1)
    rolled = pltpu.roll(x, LANES // 2, 1)
    return jnp.where(lane < LANES // 2, -rolled, rolled)


def pack_pair(first, second):
    lane = lax.broadcasted_iota(jnp.int32, first.shape, 1)
    lower = jnp.where(lane < QUAD, first, pltpu.roll(first, LANES - QUAD, 1))
    upper = jnp.where(lane < LANES - QUAD, pltpu.roll(second, PAIR, 1), pltpu.roll(second, QUAD, 1))
    return jnp.where(lane < PAIR, lower, upper)


def kept_rows(x):
    return jnp.concatenate([x[: M // 2], x[x.shape[0] - M // 2 :]], 0)


def iteration_kernel(
    edges,
    start, fine_spread, fine_gather, deep, coarse_spread, coarse_gather,
    result,
    state, fine_end, fine_out_f, fine_in_f, fine_out_b, fine_in_b,
    coarse_start, inverses, dampings, states, terms, term, landed,
    own_out_f, own_in_f, own_out_b, own_in_b, out_f, in_f, out_b, in_b,
    fine_f_send, fine_f_recv, fine_b_send, fine_b_recv,
    end_send, end_recv, term_send, term_recv, state_send, state_recv,
    own_f_send, own_f_recv, own_b_send, own_b_recv, f_send, f_recv, b_send, b_recv,
):
    slot, py, pz = lax.axis_index("tm"), lax.axis_index("py"), lax.axis_index("pz")
    slices = lax.axis_size("tm")
    stride = slices // 4
    side = slot // stride
    me = py * 4 + pz
    is_chain = (pz == 0) & (slot % stride == 0)
    own_term = (slot == 0) & (pz == 0)
    sends_term = jnp.logical_not(own_term) & (slot < slices - 1)
    fine_inverse, fine_back, inverse_pair, forward_pair, forward_one = [
        deep.at[pl.ds(low, high - low), :] for low, high in zip(edges, edges[1:])
    ]
    points, kept = G, M
    mats = (
        coarse_spread[:points], coarse_gather[:kept],
        inverse_pair[...], forward_pair[...], forward_one[...],
    )
    spread_x, gather_x = coarse_spread[points:], coarse_gather[kept:]

    def place_wave(place, length):
        return jnp.where(place < length // 2, place, place - length).astype(jnp.float32)

    coarse_shape = (M, LANES)
    coarse_kx = place_wave(lax.broadcasted_iota(jnp.int32, coarse_shape, 0), M)
    coarse_kz = (lax.broadcasted_iota(jnp.int32, coarse_shape, 1) % QUAD).astype(jnp.float32)
    members = (me, py * 4 + side)

    def coarse_ky(which):
        return lambda a: place_wave(a * PARTS + members[which], M)

    def tables_of(which):
        return (coarse_kx, coarse_ky(which), coarse_kz, inverses.at[which], dampings.at[which])

    for which in range(2):
        for a in range(LOCAL):
            ky = coarse_ky(which)(a)
            squared = coarse_kx * coarse_kx + ky * ky + coarse_kz * coarse_kz
            inverses[which, a] = 1.0 / jnp.maximum(squared, 1.0)
            dampings[which, a] = jnp.exp(-viscosity * time_step * squared)

    def slice_device(peer):
        return (slot, peer // 4, peer % 4)

    def chain_device(peer):
        return (peer % 4 * stride, peer // 4, 0)

    def for_peers(who, act, once=5):
        def some(i, carried):
            for u in range(once):
                act((who + 1 + once * i + u) % PARTS)
            return carried

        lax.fori_loop(0, (PARTS - 1) // once, some, 0)

    def term_copy(source_slice):
        return pltpu.make_async_remote_copy(
            src_ref=term,
            dst_ref=terms.at[source_slice],
            send_sem=term_send,
            recv_sem=term_recv.at[source_slice],
            device_id=(pz * stride, py, 0),
            device_id_type=MESH,
        )

    def state_copy(t):
        return pltpu.make_async_remote_copy(
            src_ref=states.at[t],
            dst_ref=landed,
            send_sem=state_send.at[t],
            recv_sem=state_recv,
            device_id=(t, py, side),
            device_id_type=MESH,
        )

    def advance_parts(state, tables, me, device_of, buffers, sems, write, compact):
        out_f, in_f, out_b, in_b = buffers
        f_send, f_recv, b_send, b_recv = sems

        def send(source, target, sends, recvs, rows, k):
            def piece(which):
                return pl.ds(pl.multiple_of((which * PIECES + k) * rows, 8), rows)

            def one(peer):
                pltpu.make_async_remote_copy(
                    src_ref=source.at[piece(peer), :],
                    dst_ref=target.at[piece(me), :],
                    send_sem=sends.at[k],
                    recv_sem=recvs.at[k],
                    device_id=device_of(peer),
                    device_id_type=MESH,
                ).start()

            for_peers(me, one, 1 if compact else 5)
            target[piece(me), :] = source[piece(me), :]

        def drain(buffer, sems, rows, k):
            bulk = buffer.at[pl.ds(0, rows * (PARTS - 1)), :]
            pltpu.make_async_copy(bulk, bulk, sems.at[k]).wait()

        forth = (out_f, in_f, f_send, f_recv, F_ROWS)
        back = (out_b, in_b, b_send, b_recv, B_ROWS)
        def begin():
            for a in range(LOCAL):
                waves = spread_waves(state, a, tables, spread_x)
                for g in range(3):
                    for h in range(2):
                        out_f[pl.ds(8 * g + LOCAL * h + a, G // 2, stride=F_ROWS), :] = waves[
                            G // 2 * h : G // 2 * (h + 1), LANES * g : LANES * (g + 1)
                        ]
            for k in range(PIECES):
                send(*forth, k)

        def piece_work(k):
            drain(in_f, f_recv, F_ROWS, k)
            for h in range(2):
                made = plane_product(in_f, k, h, mats)
                for g in range(2):
                    for a in range(LOCAL):
                        first_row = B_ROWS * k + 8 * g + LOCAL * h + a
                        out_b[pl.ds(first_row, PARTS, stride=B_ROWS * PIECES), :] = made[
                            PARTS * a : PARTS * (a + 1), LANES * g : LANES * (g + 1)
                        ]
            send(*back, k)

        def middle():
            if compact:
                def turn_of(k, carried):
                    piece_work(k)
                    return carried

                lax.fori_loop(0, PIECES, turn_of, 0)
            else:
                for k in range(PIECES):
                    piece_work(k)

        def end():
            for k in range(PIECES):
                drain(out_f, f_send, F_ROWS, k)
            for k in range(PIECES):
                drain(in_b, b_recv, B_ROWS, k)
            for a in range(LOCAL):
                write(a, *gather_waves(in_b, state, a, tables, gather_x))
            for k in range(PIECES):
                drain(out_b, b_send, B_ROWS, k)

        return begin, middle, end

    def write_own(a, first, third):
        term[a, :, :LANES] = first
        term[a, :, LANES:] = third

    own_begin, own_middle, own_end = advance_parts(
        coarse_start,
        tables_of(0),
        me,
        slice_device,
        (own_out_f, own_in_f, own_out_b, own_in_b),
        (own_f_send, own_f_recv, own_b_send, own_b_recv),
        write_own,
        compact=True,
    )

    modes = start.shape[1] // FINE_LOCAL
    planes = fine_in_f.shape[0]
    extent = planes * PARTS
    shape = (modes, LANES)
    rows = lax.broadcasted_iota(jnp.int32, shape, 0)
    kx = jnp.where(rows < modes // 2, rows, rows - modes).astype(jnp.float32)
    kz = (lax.broadcasted_iota(jnp.int32, shape, 1) % (LANES // 2)).astype(jnp.float32)

    def wave_y(a):
        place = a * PARTS + me
        return jnp.where(place < modes // 2, place, place - modes).astype(jnp.float32)

    def without_divergence(fields, ky, squared):
        divergence = (kx * fields[0] + ky * fields[1] + kz * fields[2]) / jnp.maximum(squared, 1.0)
        return (
            fields[0] - kx * divergence,
            fields[1] - ky * divergence,
            fields[2] - kz * divergence,
        )

    kept_places = (*range(LOCAL // 2), *range(FINE_LOCAL - LOCAL // 2, FINE_LOCAL))
    for a in range(FINE_LOCAL):
        ky = wave_y(a)
        squared = kx * kx + ky * ky + kz * kz
        picked = pl.ds(a, modes, stride=FINE_LOCAL)
        fields = without_divergence([start[c, picked, :] for c in range(3)], ky, squared)
        for c in range(3):
            state[c, picked, :] = fields[c]
        if a in kept_places:
            slim = [kept_rows(v) for v in fields]
            coarse_start[kept_places.index(a), :, :LANES] = pack_pair(slim[0], slim[1])
            coarse_start[kept_places.index(a), :, LANES:] = pack_pair(slim[2], slim[2])
        turned = [half_turn(v) for v in fields]
        wide = jnp.concatenate([*fields, kx * fields[1], kx * fields[2]], 1)
        wide_turned = jnp.concatenate([*turned, kx * turned[1], kx * turned[2]], 1)
        waves = left_apply(fine_spread[...], jnp.concatenate([wide, wide_turned], 0))
        for c in range(5):
            fine_out_f[pl.ds(8 * c + a, extent, stride=FINE_F), :] = waves[:, LANES * c : LANES * (c + 1)]

    def send_plane(x, carried):
        def one(peer):
            first = pl.multiple_of((peer * planes + x) * FINE_F, 8)
            pltpu.make_async_remote_copy(
                src_ref=fine_out_f.at[pl.ds(first, FINE_F), :],
                dst_ref=fine_in_f.at[x, pl.ds(pl.multiple_of(me * FINE_F, 8), FINE_F), :],
                send_sem=fine_f_send,
                recv_sem=fine_f_recv.at[x],
                device_id=slice_device(peer),
                device_id_type=MESH,
            ).start()

        for_peers(me, one, 3)
        mine = pl.multiple_of((me * planes + x) * FINE_F, 8)
        fine_in_f[x, pl.ds(pl.multiple_of(me * FINE_F, 8), FINE_F), :] = fine_out_f[pl.ds(mine, FINE_F), :]
        return carried

    own_begin()
    lax.fori_loop(0, planes, send_plane, 0)
    own_middle()
    places = lax.broadcasted_iota(jnp.int32, shape, 0)
    ky_rows = jnp.where(places < modes // 2, places, places - modes).astype(jnp.float32)

    def plane(x, carried):
        bulk = fine_in_f.at[x, pl.ds(0, FINE_F * (PARTS - 1)), :]
        pltpu.make_async_copy(bulk, bulk, fine_f_recv.at[x]).wait()
        arrived = [
            jnp.concatenate(
                [fine_in_f[x, pl.ds(8 * c + a, PARTS, stride=FINE_F), :] for a in range(FINE_LOCAL)], 0
            )
            for c in range(5)
        ]
        raw = [
            ky_rows * arrived[2] - kz * arrived[1],
            kz * arrived[0] - arrived[4],
            arrived[3] - ky_rows * arrived[0],
        ]
        fields = jnp.concatenate(arrived[:3] + [half_turn(w) for w in raw], 1)
        turned = jnp.concatenate([half_turn(v) for v in arrived[:3]] + [-w for w in raw], 1)
        along_y = left_apply(fine_spread[...], jnp.concatenate([fields, turned], 0))
        u0, u1, u2, w0, w1, w2 = [
            right_apply(along_y[:, LANES * c : LANES * (c + 1)], fine_inverse[...]) for c in range(6)
        ]
        back = [
            right_apply(n, fine_back[...])
            for n in (u1 * w2 - u2 * w1, u2 * w0 - u0 * w2, u0 * w1 - u1 * w0)
        ]
        made = left_apply(
            fine_gather[...],
            jnp.concatenate(
                [
                    jnp.concatenate([b[:, :LANES] for b in back], 1),
                    jnp.concatenate([b[:, LANES:] for b in back], 1),
                ],
                0,
            ),
        )
        for c in range(3):
            for a in range(FINE_LOCAL):
                fine_out_b[x, pl.ds(8 * c + a, PARTS, stride=FINE_B), :] = made[
                    PARTS * a : PARTS * (a + 1), LANES * c : LANES * (c + 1)
                ]
        home = pl.ds(pl.multiple_of((me * planes + x) * FINE_B, 8), FINE_B)

        def one(peer):
            pltpu.make_async_remote_copy(
                src_ref=fine_out_b.at[x, pl.ds(pl.multiple_of(peer * FINE_B, 8), FINE_B), :],
                dst_ref=fine_in_b.at[home, :],
                send_sem=fine_b_send,
                recv_sem=fine_b_recv,
                device_id=slice_device(peer),
                device_id_type=MESH,
            ).start()

        for_peers(me, one, 3)
        fine_in_b[home, :] = fine_out_b[x, pl.ds(pl.multiple_of(me * FINE_B, 8), FINE_B), :]
        return carried

    lax.fori_loop(0, planes, plane, 0)
    own_end()
    sent = fine_out_f.at[pl.ds(0, planes * (PARTS - 1) * FINE_F), :]
    pltpu.make_async_copy(sent, sent, fine_f_send).wait()
    bulk = fine_in_b.at[pl.ds(0, planes * (PARTS - 1) * FINE_B), :]
    pltpu.make_async_copy(bulk, bulk, fine_b_recv).wait()
    for a in range(FINE_LOCAL):
        ky = wave_y(a)
        squared = kx * kx + ky * ky + kz * kz
        picked = pl.ds(a, modes, stride=FINE_LOCAL)
        columns = [fine_in_b[pl.ds(8 * c + a, extent, stride=FINE_B), :] for c in range(3)]
        turned = [half_turn(v) for v in columns]
        narrow = left_apply(
            fine_gather[...],
            jnp.concatenate([jnp.concatenate(columns, 1), jnp.concatenate(turned, 1)], 0),
        )
        pushed = without_divergence(
            [narrow[:, LANES * c : LANES * (c + 1)] for c in range(3)], ky, squared
        )
        damping = jnp.exp(-viscosity * time_step * squared)
        ends = [damping * (state[c, picked, :] + time_step * pushed[c]) for c in range(3)]
        for c in range(3):
            fine_end[c, picked, :] = ends[c]
        if a in kept_places:
            place = kept_places.index(a)
            slim = [kept_rows(v) for v in ends]
            for half, low in ((0, pack_pair(slim[0], slim[1])), (LANES, pack_pair(slim[2], slim[2]))):
                lanes = pl.ds(half, LANES)
                term[place, :, lanes] = low - jnp.where(slot == 0, 0.0, term[place, :, lanes])
    pltpu.make_async_copy(bulk, bulk, fine_b_send).wait()

    end_copy = pltpu.make_async_remote_copy(
        src_ref=fine_end,
        dst_ref=result,
        send_sem=end_send,
        recv_sem=end_recv,
        device_id=((slot + 1) % slices, py, pz),
        device_id_type=MESH,
    )

    @pl.when(sends_term)
    def _():
        term_copy(slot).start()

    @pl.when(slot < slices - 1)
    def _():
        end_copy.start()

    @pl.when(is_chain)
    def _():
        @pl.when(own_term)
        def _():
            states[1] = term[...]

        @pl.when(jnp.logical_not(own_term))
        def _():
            term_copy(0).wait_recv()
            states[1] = terms[0]

        def step(t, carried):
            def write_state(a, first, third):
                if a == 0:
                    term_copy(t).wait_recv()
                states[t + 1, a, :, :LANES] = first + terms[t, a, :, :LANES]
                states[t + 1, a, :, LANES:] = third + terms[t, a, :, LANES:]

            begin, middle, end = advance_parts(
                states.at[t],
                tables_of(1),
                members[1],
                chain_device,
                (out_f, in_f, out_b, in_b),
                (f_send, f_recv, b_send, b_recv),
                write_state,
                compact=False,
            )
            begin()
            state_copy(t).start()
            middle()
            end()
            return carried

        lax.fori_loop(1, slices - 1, step, 0)
        state_copy(slices - 1).start()

        def finish_state(t, carried):
            state_copy(t).wait_send()
            return carried

        lax.fori_loop(1, slices, finish_state, 0)

    @pl.when(sends_term)
    def _():
        term_copy(slot).wait_send()

    @pl.when(slot < slices - 1)
    def _():
        end_copy.wait_send()

    @pl.when(slot == 0)
    def _():
        result[...] = state[...]

    @pl.when(slot != 0)
    def _():
        state_copy(slot).wait_recv()
        end_copy.wait_recv()
        half = M // 2
        lane = lax.broadcasted_iota(jnp.int32, (half, LANES), 1)
        real, imaginary = lane < QUAD, (lane >= PAIR) & (lane < PAIR + QUAD)
        for place, a in enumerate(kept_places):
            for top, first in ((0, 0), (half, modes - half)):
                pair = landed[place, pl.ds(top, half), :LANES]
                single = landed[place, pl.ds(top, half), LANES:]
                moved = (
                    (pair, pltpu.roll(pair, QUAD, 1)),
                    (pltpu.roll(pair, PAIR, 1), pltpu.roll(pair, LANES - QUAD, 1)),
                    (single, pltpu.roll(single, QUAD, 1)),
                )
                rows = pl.ds(first * FINE_LOCAL + a, half, stride=FINE_LOCAL)
                for c in range(3):
                    result[c, rows, :] = jnp.where(
                        real, moved[c][0], jnp.where(imaginary, moved[c][1], result[c, rows, :])
                    )


def shards(start_states):
    retained = start_states.shape[-1]
    extent = 3 * retained // 2
    planes = extent // PARTS
    slices = lax.axis_size("tm")
    matrices, edges = transforms(retained)
    operands = [start_states.reshape(3, retained * FINE_LOCAL, LANES), *matrices]
    vmem = pl.BlockSpec(memory_space=pltpu.VMEM)

    def floats(*shape):
        return pltpu.VMEM(shape, jnp.float32)

    block = (LOCAL, M, 2 * LANES)
    wide = floats(PARTS * PIECES * F_ROWS, LANES)
    narrow = floats(PARTS * PIECES * B_ROWS, LANES)
    single = pltpu.SemaphoreType.DMA
    pieces = pltpu.SemaphoreType.DMA((PIECES,))
    each = pltpu.SemaphoreType.DMA((slices,))
    result = pl.pallas_call(
        partial(iteration_kernel, edges),
        out_shape=jax.ShapeDtypeStruct(operands[0].shape, jnp.float32),
        in_specs=[vmem] * len(operands),
        out_specs=vmem,
        scratch_shapes=[
            floats(*operands[0].shape), floats(*operands[0].shape),
            floats(extent * FINE_F, LANES), floats(planes, PARTS * FINE_F, LANES),
            floats(planes, PARTS * FINE_B, LANES), floats(extent * FINE_B, LANES),
            floats(*block), floats(2, LOCAL, M, LANES), floats(2, LOCAL, M, LANES),
            floats(slices, *block), floats(slices, *block), floats(*block), floats(*block),
            wide, wide, narrow, narrow, wide, wide, narrow, narrow,
            single, pltpu.SemaphoreType.DMA((planes,)), single, single,
            single, single, single, each, each, single,
            pieces, pieces, pieces, pieces, pieces, pieces, pieces, pieces,
        ],
        compiler_params=pltpu.CompilerParams(
            has_side_effects=True, vmem_limit_bytes=56 * 1024 * 1024
        ),
    )(*operands)
    return result.reshape(start_states.shape)


def solution(mesh):
    in_specs = (P("tm", None, None, None, ("py", "pz"), None),)
    out_specs = P("tm", None, None, None, ("py", "pz"), None)
    return jax.shard_map(shards, mesh=mesh, in_specs=in_specs, out_specs=out_specs, check_vma=False)
```

```python
from functools import partial

import jax
import jax.numpy as jnp
from jax import lax
from jax.experimental import pallas as pl
from jax.experimental.pallas import tpu as pltpu
import numpy as np
from jax.sharding import PartitionSpec as P

M = 64


viscosity = 0.03
time_step = 0.004


G = 3 * M // 2
PARTS = 16
LOCAL = M // PARTS
PLANES = G // PARTS
PIECES = PLANES // 2
FINE_LOCAL = 8
FINE_F = 5 * FINE_LOCAL
FINE_B = 3 * FINE_LOCAL
F_ROWS = 24
B_ROWS = 16
LANES = 128
PAIR = LANES // 2
QUAD = PAIR // 2
MESH = pl.DeviceIdType.MESH


def halves(matrix):
    high = np.asarray(matrix, np.float32).astype(jnp.bfloat16)
    low = (np.asarray(matrix, np.float32) - high.astype(np.float32)).astype(jnp.bfloat16)
    return high, low


def stacked(matrix, axis):
    high, low = halves(matrix)
    return jnp.asarray(np.concatenate([high, high, low], axis))


def transform_pair(retained):
    extent = 3 * retained // 2
    points = np.arange(extent)
    waves = np.where(np.arange(retained) < retained // 2, np.arange(retained), np.arange(retained) - retained)
    angle = (points[:, None] * waves[None, :]) % extent * (2.0 * np.pi / extent)
    spread = np.concatenate([np.cos(angle), np.sin(angle)], 1) * retained**-0.5
    gather = np.concatenate([np.cos(angle.T), -np.sin(angle.T)], 1) * (retained**0.5 / extent)
    return spread, gather


def depth_transforms(retained, lanes):
    extent, half = 3 * retained // 2, retained // 2
    points, harmonic = np.arange(extent), np.arange(half)
    angle = (points[:, None] * harmonic[None, :]) % extent * (2.0 * np.pi / extent)
    weight = np.where(harmonic == 0, 1.0, 2.0) * retained**-0.5
    inverse = np.zeros((retained, lanes))
    inverse[:, :extent] = np.concatenate([np.cos(angle) * weight, -np.sin(angle) * weight], 1).T
    forward = np.zeros((lanes, retained))
    forward[:extent] = np.concatenate([np.cos(angle), -np.sin(angle)], 1) * (retained**0.5 / extent)
    turned = np.concatenate([-forward[:, half:], forward[:, :half]], 1)
    return inverse, forward, turned


def transforms(retained):
    spread, gather = transform_pair(M)
    inverse, forward, turned = depth_transforms(M, LANES)
    none_in = np.zeros_like(inverse)
    none_out = np.zeros_like(forward)
    inverse_pair = np.block([[inverse, none_in], [none_in, inverse]])
    forward_pair = np.block(
        [[forward, none_out, turned, none_out], [none_out, forward, none_out, turned]]
    )
    forward_one = np.concatenate([forward, forward, turned, turned], 1)
    order = np.concatenate([np.arange(0, G, 2), np.arange(1, G, 2)])
    gather_rows = np.concatenate([gather[:, order], gather[:, G + order]], 1)
    fine_spread, fine_gather = transform_pair(retained)
    fine_inverse, fine_forward, fine_turned = depth_transforms(retained, 2 * LANES)
    fine_back = np.concatenate([fine_forward, fine_turned], 1)
    deep = [stacked(m, 0) for m in (fine_inverse, fine_back, inverse_pair, forward_pair, forward_one)]
    edges = np.cumsum([0] + [m.shape[0] for m in deep]).tolist()
    operands = [
        stacked(fine_spread, 1),
        stacked(fine_gather, 1),
        jnp.concatenate(deep, 0),
        jnp.concatenate([stacked(spread, 1), stacked(spread[order], 1)], 0),
        jnp.concatenate([stacked(gather, 1), stacked(gather_rows, 1)], 0),
    ]
    return operands, edges


def turn(x):
    lane = lax.broadcasted_iota(jnp.int32, x.shape, 1)
    return jnp.where(
        lane % PAIR < QUAD, -pltpu.roll(x, LANES - QUAD, 1), pltpu.roll(x, QUAD, 1)
    )


def split(x):
    high = x.astype(jnp.bfloat16)
    return high, (x - high.astype(jnp.float32)).astype(jnp.bfloat16)


def left_apply(matrix, x):
    high, low = split(x)
    return jnp.dot(
        matrix, jnp.concatenate([high, low, high], 0), preferred_element_type=jnp.float32
    )


def right_apply(x, matrix):
    high, low = split(x)
    return jnp.dot(
        jnp.concatenate([high, low, high], 1), matrix, preferred_element_type=jnp.float32
    )


def spread_waves(state, a, tables, spread):
    kx, ky, kz = tables[0], tables[1](a), tables[2]
    first, third = state[a, :, :LANES], state[a, :, LANES:]
    lower = lax.broadcasted_iota(jnp.int32, first.shape, 1) < PAIR
    kxy, kzx = jnp.where(lower, kx, ky), jnp.where(lower, kz, kx)
    raw_one = ky * third - kz * first
    raw_two = kzx * first - kxy * jnp.where(lower, third, pltpu.roll(first, PAIR, 1))
    fields = jnp.concatenate(
        [first, jnp.where(lower, third, turn(raw_one)), turn(raw_two)], 1
    )
    turned = jnp.concatenate(
        [turn(first), jnp.where(lower, turn(third), -raw_one), -raw_two], 1
    )
    return left_apply(spread, jnp.concatenate([fields, turned], 0))


def plane_product(fetched, k, h, mats):
    spread, gather, inverse_pair, forward_pair, forward_one = mats
    fields, turned = [], []
    for g in range(3):
        rows = jnp.concatenate(
            [
                fetched[
                    pl.ds(
                        F_ROWS * k + 8 * g + LOCAL * h + a,
                        PARTS,
                        stride=F_ROWS * PIECES,
                    ),
                    :,
                ]
                for a in range(LOCAL)
            ],
            0,
        )
        fields.append(rows)
        turned.append(turn(rows))
    along_y = left_apply(
        spread, jnp.concatenate([jnp.concatenate(fields, 1), jnp.concatenate(turned, 1)], 0)
    )
    grids = [
        right_apply(along_y[:, LANES * g : LANES * (g + 1)], inverse_pair) for g in range(3)
    ]
    u0, u1 = grids[0][:, :LANES], grids[0][:, LANES:]
    u2, w0 = grids[1][:, :LANES], grids[1][:, LANES:]
    w1, w2 = grids[2][:, :LANES], grids[2][:, LANES:]
    pair = jnp.concatenate([u1 * w2 - u2 * w1, u2 * w0 - u0 * w2], 1)
    back_pair = right_apply(pair, forward_pair)
    back_one = right_apply(u0 * w1 - u1 * w0, forward_one)
    return left_apply(
        gather,
        jnp.concatenate(
            [
                jnp.concatenate([back_pair[:, :LANES], back_one[:, :LANES]], 1),
                jnp.concatenate([back_pair[:, LANES:], back_one[:, LANES:]], 1),
            ],
            0,
        ),
    )


def gather_waves(fetched, state, a, tables, gather):
    kx, ky, kz, inverse, damping = tables[0], tables[1](a), tables[2], tables[3][a], tables[4][a]
    kxy = jnp.where(lax.broadcasted_iota(jnp.int32, kx.shape, 1) < PAIR, kx, ky)
    rows = [
        jnp.concatenate(
            [
                fetched[pl.ds(8 * g + LOCAL * h + a, G // 2, stride=B_ROWS), :]
                for h in range(2)
            ],
            0,
        )
        for g in range(2)
    ]
    turned = [turn(r) for r in rows]
    modes = left_apply(
        gather, jnp.concatenate([jnp.concatenate(rows, 1), jnp.concatenate(turned, 1)], 0)
    )
    first, third = modes[:, :LANES], modes[:, LANES:]
    along = kxy * first
    divergence = (along + pltpu.roll(along, PAIR, 1) + kz * third) * inverse
    return (
        damping * (state[a, :, :LANES] + time_step * (first - kxy * divergence)),
        damping * (state[a, :, LANES:] + time_step * (third - kz * divergence)),
    )


def half_turn(x):
    lane = lax.broadcasted_iota(jnp.int32, x.shape, 1)
    rolled = pltpu.roll(x, LANES // 2, 1)
    return jnp.where(lane < LANES // 2, -rolled, rolled)


def pack_pair(first, second):
    lane = lax.broadcasted_iota(jnp.int32, first.shape, 1)
    lower = jnp.where(lane < QUAD, first, pltpu.roll(first, LANES - QUAD, 1))
    upper = jnp.where(lane < LANES - QUAD, pltpu.roll(second, PAIR, 1), pltpu.roll(second, QUAD, 1))
    return jnp.where(lane < PAIR, lower, upper)


def kept_rows(x):
    return jnp.concatenate([x[: M // 2], x[x.shape[0] - M // 2 :]], 0)


def iteration_kernel(
    edges,
    start, fine_spread, fine_gather, deep, coarse_spread, coarse_gather,
    result,
    state, fine_end, fine_out_f, fine_in_f, fine_out_b, fine_in_b,
    coarse_start, inverses, dampings, states, terms, term, landed,
    own_out_f, own_in_f, own_out_b, own_in_b, out_f, in_f, out_b, in_b,
    fine_f_send, fine_f_recv, fine_b_send, fine_b_recv,
    end_send, end_recv, term_send, term_recv, state_send, state_recv,
    own_f_send, own_f_recv, own_b_send, own_b_recv, f_send, f_recv, b_send, b_recv,
):
    slot, py, pz = lax.axis_index("tm"), lax.axis_index("py"), lax.axis_index("pz")
    slices = lax.axis_size("tm")
    stride = slices // 4
    side = slot // stride
    me = py * 4 + pz
    is_chain = (pz == 0) & (slot % stride == 0)
    own_term = (slot == 0) & (pz == 0)
    sends_term = jnp.logical_not(own_term) & (slot < slices - 1)
    fine_inverse, fine_back, inverse_pair, forward_pair, forward_one = [
        deep.at[pl.ds(low, high - low), :] for low, high in zip(edges, edges[1:])
    ]
    points, kept = G, M
    mats = (
        coarse_spread[:points], coarse_gather[:kept],
        inverse_pair[...], forward_pair[...], forward_one[...],
    )
    spread_x, gather_x = coarse_spread[points:], coarse_gather[kept:]

    def place_wave(place, length):
        return jnp.where(place < length // 2, place, place - length).astype(jnp.float32)

    coarse_shape = (M, LANES)
    coarse_kx = place_wave(lax.broadcasted_iota(jnp.int32, coarse_shape, 0), M)
    coarse_kz = (lax.broadcasted_iota(jnp.int32, coarse_shape, 1) % QUAD).astype(jnp.float32)
    members = (me, py * 4 + side)

    def coarse_ky(which):
        return lambda a: place_wave(a * PARTS + members[which], M)

    def tables_of(which):
        return (coarse_kx, coarse_ky(which), coarse_kz, inverses.at[which], dampings.at[which])

    for which in range(2):
        for a in range(LOCAL):
            ky = coarse_ky(which)(a)
            squared = coarse_kx * coarse_kx + ky * ky + coarse_kz * coarse_kz
            inverses[which, a] = 1.0 / jnp.maximum(squared, 1.0)
            dampings[which, a] = jnp.exp(-viscosity * time_step * squared)

    def slice_device(peer):
        return (slot, peer // 4, peer % 4)

    def chain_device(peer):
        return (peer % 4 * stride, peer // 4, 0)

    def for_peers(who, act, once=5):
        def some(i, carried):
            for u in range(once):
                act((who + 1 + once * i + u) % PARTS)
            return carried

        lax.fori_loop(0, (PARTS - 1) // once, some, 0)

    def term_copy(source_slice):
        return pltpu.make_async_remote_copy(
            src_ref=term,
            dst_ref=terms.at[source_slice],
            send_sem=term_send,
            recv_sem=term_recv.at[source_slice],
            device_id=(pz * stride, py, 0),
            device_id_type=MESH,
        )

    def state_copy(t):
        return pltpu.make_async_remote_copy(
            src_ref=states.at[t],
            dst_ref=landed,
            send_sem=state_send.at[t],
            recv_sem=state_recv,
            device_id=(t, py, side),
            device_id_type=MESH,
        )

    def advance_parts(state, tables, me, device_of, buffers, sems, write, compact):
        out_f, in_f, out_b, in_b = buffers
        f_send, f_recv, b_send, b_recv = sems

        def send(source, target, sends, recvs, rows, k):
            def piece(which):
                return pl.ds(pl.multiple_of((which * PIECES + k) * rows, 8), rows)

            def one(peer):
                pltpu.make_async_remote_copy(
                    src_ref=source.at[piece(peer), :],
                    dst_ref=target.at[piece(me), :],
                    send_sem=sends.at[k],
                    recv_sem=recvs.at[k],
                    device_id=device_of(peer),
                    device_id_type=MESH,
                ).start()

            for_peers(me, one, 1 if compact else 5)
            target[piece(me), :] = source[piece(me), :]

        def drain(buffer, sems, rows, k):
            bulk = buffer.at[pl.ds(0, rows * (PARTS - 1)), :]
            pltpu.make_async_copy(bulk, bulk, sems.at[k]).wait()

        forth = (out_f, in_f, f_send, f_recv, F_ROWS)
        back = (out_b, in_b, b_send, b_recv, B_ROWS)
        def begin():
            for a in range(LOCAL):
                waves = spread_waves(state, a, tables, spread_x)
                for g in range(3):
                    for h in range(2):
                        out_f[pl.ds(8 * g + LOCAL * h + a, G // 2, stride=F_ROWS), :] = waves[
                            G // 2 * h : G // 2 * (h + 1), LANES * g : LANES * (g + 1)
                        ]
            for k in range(PIECES):
                send(*forth, k)

        def piece_work(k):
            drain(in_f, f_recv, F_ROWS, k)
            for h in range(2):
                made = plane_product(in_f, k, h, mats)
                for g in range(2):
                    for a in range(LOCAL):
                        first_row = B_ROWS * k + 8 * g + LOCAL * h + a
                        out_b[pl.ds(first_row, PARTS, stride=B_ROWS * PIECES), :] = made[
                            PARTS * a : PARTS * (a + 1), LANES * g : LANES * (g + 1)
                        ]
            send(*back, k)

        def middle():
            if compact:
                def turn_of(k, carried):
                    piece_work(k)
                    return carried

                lax.fori_loop(0, PIECES, turn_of, 0)
            else:
                for k in range(PIECES):
                    piece_work(k)

        def end():
            for k in range(PIECES):
                drain(out_f, f_send, F_ROWS, k)
            for k in range(PIECES):
                drain(in_b, b_recv, B_ROWS, k)
            for a in range(LOCAL):
                write(a, *gather_waves(in_b, state, a, tables, gather_x))
            for k in range(PIECES):
                drain(out_b, b_send, B_ROWS, k)

        return begin, middle, end

    def write_own(a, first, third):
        term[a, :, :LANES] = first
        term[a, :, LANES:] = third

    own_begin, own_middle, own_end = advance_parts(
        coarse_start,
        tables_of(0),
        me,
        slice_device,
        (own_out_f, own_in_f, own_out_b, own_in_b),
        (own_f_send, own_f_recv, own_b_send, own_b_recv),
        write_own,
        compact=True,
    )

    modes = start.shape[1] // FINE_LOCAL
    planes = fine_in_f.shape[0]
    extent = planes * PARTS
    shape = (modes, LANES)
    rows = lax.broadcasted_iota(jnp.int32, shape, 0)
    kx = jnp.where(rows < modes // 2, rows, rows - modes).astype(jnp.float32)
    kz = (lax.broadcasted_iota(jnp.int32, shape, 1) % (LANES // 2)).astype(jnp.float32)

    def wave_y(a):
        place = a * PARTS + me
        return jnp.where(place < modes // 2, place, place - modes).astype(jnp.float32)

    def without_divergence(fields, ky, squared):
        divergence = (kx * fields[0] + ky * fields[1] + kz * fields[2]) / jnp.maximum(squared, 1.0)
        return (
            fields[0] - kx * divergence,
            fields[1] - ky * divergence,
            fields[2] - kz * divergence,
        )

    kept_places = (*range(LOCAL // 2), *range(FINE_LOCAL - LOCAL // 2, FINE_LOCAL))
    for a in range(FINE_LOCAL):
        ky = wave_y(a)
        squared = kx * kx + ky * ky + kz * kz
        picked = pl.ds(a, modes, stride=FINE_LOCAL)
        fields = without_divergence([start[c, picked, :] for c in range(3)], ky, squared)
        for c in range(3):
            state[c, picked, :] = fields[c]
        if a in kept_places:
            slim = [kept_rows(v) for v in fields]
            coarse_start[kept_places.index(a), :, :LANES] = pack_pair(slim[0], slim[1])
            coarse_start[kept_places.index(a), :, LANES:] = pack_pair(slim[2], slim[2])
        turned = [half_turn(v) for v in fields]
        wide = jnp.concatenate([*fields, kx * fields[1], kx * fields[2]], 1)
        wide_turned = jnp.concatenate([*turned, kx * turned[1], kx * turned[2]], 1)
        waves = left_apply(fine_spread[...], jnp.concatenate([wide, wide_turned], 0))
        for c in range(5):
            fine_out_f[pl.ds(8 * c + a, extent, stride=FINE_F), :] = waves[:, LANES * c : LANES * (c + 1)]

    def send_plane(x, carried):
        def one(peer):
            first = pl.multiple_of((peer * planes + x) * FINE_F, 8)
            pltpu.make_async_remote_copy(
                src_ref=fine_out_f.at[pl.ds(first, FINE_F), :],
                dst_ref=fine_in_f.at[x, pl.ds(pl.multiple_of(me * FINE_F, 8), FINE_F), :],
                send_sem=fine_f_send,
                recv_sem=fine_f_recv.at[x],
                device_id=slice_device(peer),
                device_id_type=MESH,
            ).start()

        for_peers(me, one, 3)
        mine = pl.multiple_of((me * planes + x) * FINE_F, 8)
        fine_in_f[x, pl.ds(pl.multiple_of(me * FINE_F, 8), FINE_F), :] = fine_out_f[pl.ds(mine, FINE_F), :]
        return carried

    own_begin()
    lax.fori_loop(0, planes, send_plane, 0)
    own_middle()
    places = lax.broadcasted_iota(jnp.int32, shape, 0)
    ky_rows = jnp.where(places < modes // 2, places, places - modes).astype(jnp.float32)

    def plane(x, carried):
        bulk = fine_in_f.at[x, pl.ds(0, FINE_F * (PARTS - 1)), :]
        pltpu.make_async_copy(bulk, bulk, fine_f_recv.at[x]).wait()
        arrived = [
            jnp.concatenate(
                [fine_in_f[x, pl.ds(8 * c + a, PARTS, stride=FINE_F), :] for a in range(FINE_LOCAL)], 0
            )
            for c in range(5)
        ]
        raw = [
            ky_rows * arrived[2] - kz * arrived[1],
            kz * arrived[0] - arrived[4],
            arrived[3] - ky_rows * arrived[0],
        ]
        fields = jnp.concatenate(arrived[:3] + [half_turn(w) for w in raw], 1)
        turned = jnp.concatenate([half_turn(v) for v in arrived[:3]] + [-w for w in raw], 1)
        along_y = left_apply(fine_spread[...], jnp.concatenate([fields, turned], 0))
        u0, u1, u2, w0, w1, w2 = [
            right_apply(along_y[:, LANES * c : LANES * (c + 1)], fine_inverse[...]) for c in range(6)
        ]
        back = [
            right_apply(n, fine_back[...])
            for n in (u1 * w2 - u2 * w1, u2 * w0 - u0 * w2, u0 * w1 - u1 * w0)
        ]
        made = left_apply(
            fine_gather[...],
            jnp.concatenate(
                [
                    jnp.concatenate([b[:, :LANES] for b in back], 1),
                    jnp.concatenate([b[:, LANES:] for b in back], 1),
                ],
                0,
            ),
        )
        for c in range(3):
            for a in range(FINE_LOCAL):
                fine_out_b[x, pl.ds(8 * c + a, PARTS, stride=FINE_B), :] = made[
                    PARTS * a : PARTS * (a + 1), LANES * c : LANES * (c + 1)
                ]
        home = pl.ds(pl.multiple_of((me * planes + x) * FINE_B, 8), FINE_B)

        def one(peer):
            pltpu.make_async_remote_copy(
                src_ref=fine_out_b.at[x, pl.ds(pl.multiple_of(peer * FINE_B, 8), FINE_B), :],
                dst_ref=fine_in_b.at[home, :],
                send_sem=fine_b_send,
                recv_sem=fine_b_recv,
                device_id=slice_device(peer),
                device_id_type=MESH,
            ).start()

        for_peers(me, one, 3)
        fine_in_b[home, :] = fine_out_b[x, pl.ds(pl.multiple_of(me * FINE_B, 8), FINE_B), :]
        return carried

    lax.fori_loop(0, planes, plane, 0)
    own_end()
    sent = fine_out_f.at[pl.ds(0, planes * (PARTS - 1) * FINE_F), :]
    pltpu.make_async_copy(sent, sent, fine_f_send).wait()
    bulk = fine_in_b.at[pl.ds(0, planes * (PARTS - 1) * FINE_B), :]
    pltpu.make_async_copy(bulk, bulk, fine_b_recv).wait()
    for a in range(FINE_LOCAL):
        ky = wave_y(a)
        squared = kx * kx + ky * ky + kz * kz
        picked = pl.ds(a, modes, stride=FINE_LOCAL)
        columns = [fine_in_b[pl.ds(8 * c + a, extent, stride=FINE_B), :] for c in range(3)]
        turned = [half_turn(v) for v in columns]
        narrow = left_apply(
            fine_gather[...],
            jnp.concatenate([jnp.concatenate(columns, 1), jnp.concatenate(turned, 1)], 0),
        )
        pushed = without_divergence(
            [narrow[:, LANES * c : LANES * (c + 1)] for c in range(3)], ky, squared
        )
        damping = jnp.exp(-viscosity * time_step * squared)
        ends = [damping * (state[c, picked, :] + time_step * pushed[c]) for c in range(3)]
        for c in range(3):
            fine_end[c, picked, :] = ends[c]
        if a in kept_places:
            place = kept_places.index(a)
            slim = [kept_rows(v) for v in ends]
            for half, low in ((0, pack_pair(slim[0], slim[1])), (LANES, pack_pair(slim[2], slim[2]))):
                lanes = pl.ds(half, LANES)
                term[place, :, lanes] = low - jnp.where(slot == 0, 0.0, term[place, :, lanes])
    pltpu.make_async_copy(bulk, bulk, fine_b_send).wait()

    end_copy = pltpu.make_async_remote_copy(
        src_ref=fine_end,
        dst_ref=result,
        send_sem=end_send,
        recv_sem=end_recv,
        device_id=((slot + 1) % slices, py, pz),
        device_id_type=MESH,
    )

    late_term = sends_term & (slot >= 3) & jnp.logical_not(is_chain)

    @pl.when(sends_term & jnp.logical_not(late_term))
    def _():
        term_copy(slot).start()

    @pl.when(slot < slices - 1)
    def _():
        end_copy.start()

    @pl.when(late_term)
    def _():
        end_copy.wait_send()
        term_copy(slot).start()

    @pl.when(is_chain)
    def _():
        @pl.when(own_term)
        def _():
            states[1] = term[...]

        @pl.when(jnp.logical_not(own_term))
        def _():
            term_copy(0).wait_recv()
            states[1] = terms[0]

        def step(t, carried):
            def write_state(a, first, third):
                if a == 0:
                    term_copy(t).wait_recv()
                states[t + 1, a, :, :LANES] = first + terms[t, a, :, :LANES]
                states[t + 1, a, :, LANES:] = third + terms[t, a, :, LANES:]

            begin, middle, end = advance_parts(
                states.at[t],
                tables_of(1),
                members[1],
                chain_device,
                (out_f, in_f, out_b, in_b),
                (f_send, f_recv, b_send, b_recv),
                write_state,
                compact=False,
            )
            begin()
            state_copy(t).start()
            middle()
            end()
            return carried

        lax.fori_loop(1, slices - 1, step, 0)
        state_copy(slices - 1).start()

        def finish_state(t, carried):
            state_copy(t).wait_send()
            return carried

        lax.fori_loop(1, slices, finish_state, 0)

    @pl.when(sends_term)
    def _():
        term_copy(slot).wait_send()

    @pl.when((slot < slices - 1) & jnp.logical_not(late_term))
    def _():
        end_copy.wait_send()

    @pl.when(slot == 0)
    def _():
        result[...] = state[...]

    @pl.when(slot != 0)
    def _():
        state_copy(slot).wait_recv()
        end_copy.wait_recv()
        half = M // 2
        lane = lax.broadcasted_iota(jnp.int32, (half, LANES), 1)
        real, imaginary = lane < QUAD, (lane >= PAIR) & (lane < PAIR + QUAD)
        for place, a in enumerate(kept_places):
            for top, first in ((0, 0), (half, modes - half)):
                pair = landed[place, pl.ds(top, half), :LANES]
                single = landed[place, pl.ds(top, half), LANES:]
                moved = (
                    (pair, pltpu.roll(pair, QUAD, 1)),
                    (pltpu.roll(pair, PAIR, 1), pltpu.roll(pair, LANES - QUAD, 1)),
                    (single, pltpu.roll(single, QUAD, 1)),
                )
                rows = pl.ds(first * FINE_LOCAL + a, half, stride=FINE_LOCAL)
                for c in range(3):
                    result[c, rows, :] = jnp.where(
                        real, moved[c][0], jnp.where(imaginary, moved[c][1], result[c, rows, :])
                    )


def shards(start_states):
    retained = start_states.shape[-1]
    extent = 3 * retained // 2
    planes = extent // PARTS
    slices = lax.axis_size("tm")
    matrices, edges = transforms(retained)
    operands = [start_states.reshape(3, retained * FINE_LOCAL, LANES), *matrices]
    vmem = pl.BlockSpec(memory_space=pltpu.VMEM)

    def floats(*shape):
        return pltpu.VMEM(shape, jnp.float32)

    block = (LOCAL, M, 2 * LANES)
    wide = floats(PARTS * PIECES * F_ROWS, LANES)
    narrow = floats(PARTS * PIECES * B_ROWS, LANES)
    single = pltpu.SemaphoreType.DMA
    pieces = pltpu.SemaphoreType.DMA((PIECES,))
    each = pltpu.SemaphoreType.DMA((slices,))
    result = pl.pallas_call(
        partial(iteration_kernel, edges),
        out_shape=jax.ShapeDtypeStruct(operands[0].shape, jnp.float32),
        in_specs=[vmem] * len(operands),
        out_specs=vmem,
        scratch_shapes=[
            floats(*operands[0].shape), floats(*operands[0].shape),
            floats(extent * FINE_F, LANES), floats(planes, PARTS * FINE_F, LANES),
            floats(planes, PARTS * FINE_B, LANES), floats(extent * FINE_B, LANES),
            floats(*block), floats(2, LOCAL, M, LANES), floats(2, LOCAL, M, LANES),
            floats(slices, *block), floats(slices, *block), floats(*block), floats(*block),
            wide, wide, narrow, narrow, wide, wide, narrow, narrow,
            single, pltpu.SemaphoreType.DMA((planes,)), single, single,
            single, single, single, each, each, single,
            pieces, pieces, pieces, pieces, pieces, pieces, pieces, pieces,
        ],
        compiler_params=pltpu.CompilerParams(
            has_side_effects=True, vmem_limit_bytes=56 * 1024 * 1024
        ),
    )(*operands)
    return result.reshape(start_states.shape)


def solution(mesh):
    in_specs = (P("tm", None, None, None, ("py", "pz"), None),)
    out_specs = P("tm", None, None, None, ("py", "pz"), None)
    return jax.shard_map(shards, mesh=mesh, in_specs=in_specs, out_specs=out_specs, check_vma=False)
```
